8 devices in a mesh: dp: 2 (over z, y), tp: 4 (over x, core).
Axes of the slice: x: 2, y: 2, z: 1, core: 2. Of those that a mesh axis runs over, the one named last changes fastest.
Arguments:
- irreps: bfloat16 [4096, 49, 128], P('dp', None, 'tp')
- norm_gain: float32 [7, 128], P(None, 'tp')
- w_up: bfloat16 [7, 128, 256], P(None, None, 'tp')
- w_gate: bfloat16 [128, 256], P(None, 'tp')
- w_down: bfloat16 [7, 256, 128], P(None, 'tp')
- to_grid: float32 [49, 196], replicated
- from_grid: float32 [196, 48], replicated
- grad_out: bfloat16 [4096, 49, 128], P('dp', None, 'tp')
Outputs:
- output 1: bfloat16 [4096, 49, 128], P('dp', None, 'tp')
- output 2: bfloat16 [4096, 49, 128], P('dp', None, 'tp')
- output 3: bfloat16 [7, 128, 256], P(None, None, 'tp')
- output 4: bfloat16 [128, 256], P(None, 'tp')
- output 5: bfloat16 [7, 256, 128], P(None, 'tp')
All inputs are finite; a program needn't handle non-finite values.
Results may differ from the reference program's by a relative error of at most 0.0127252.
Values are sent between devices in bfloat16 or wider.
A program may use at most 1 GiB of HBM per device.

```python
import math
import jax
import jax.numpy as jnp
from jax import lax

N_NODES = 4096
CHANNELS = 128
HIDDEN = 256
DEG_MAX = 6
GRID_PTS = 196

DEGREES = DEG_MAX + 1
COEFS = DEGREES * DEGREES
ROW_BLOCK = math.gcd(N_NODES, 128)
NORM_EPS = 1e-5


def setup_inputs(seed: int = 0) -> dict:
    key_list = jax.random.split(jax.random.key(seed), 11)
    chan_pos = jnp.arange(CHANNELS, dtype=jnp.float32) / CHANNELS
    chan_scale = jnp.exp(2.4 * (chan_pos - 0.5) + 0.3 * jax.random.normal(key_list[0], (CHANNELS,)))
    node_scale = jnp.exp(0.4 * jax.random.normal(key_list[1], (N_NODES, 1, 1)))
    scalar_row = (jnp.arange(COEFS) == 0).astype(jnp.float32)[:, None]
    offsets = 0.8 * jax.random.normal(key_list[2], (CHANNELS,))
    noise_draw = jax.random.normal(key_list[3], (N_NODES, COEFS, CHANNELS))
    irreps = node_scale * chan_scale * (noise_draw + scalar_row * offsets)
    norm_gain = 0.6 + 0.8 * jax.random.uniform(key_list[4], (DEGREES, CHANNELS))
    w_up = jax.random.normal(key_list[5], (DEGREES, CHANNELS, HIDDEN)) * CHANNELS ** -0.5
    w_gate = jax.random.normal(key_list[6], (CHANNELS, HIDDEN)) * CHANNELS ** -0.5
    w_down = jax.random.normal(key_list[7], (DEGREES, HIDDEN, CHANNELS)) * HIDDEN ** -0.5
    to_grid = jax.random.normal(key_list[8], (COEFS, GRID_PTS)) * COEFS ** -0.5
    from_grid = jax.random.normal(key_list[9], (GRID_PTS, COEFS - 1)) * GRID_PTS ** -0.5
    grad_out = jax.random.normal(key_list[10], (N_NODES, COEFS, CHANNELS))
    return {'irreps': irreps.astype(jnp.bfloat16), 'norm_gain': norm_gain, 'w_up': w_up.astype(jnp.bfloat16), 'w_gate': w_gate.astype(jnp.bfloat16), 'w_down': w_down.astype(jnp.bfloat16), 'to_grid': to_grid, 'from_grid': from_grid, 'grad_out': grad_out.astype(jnp.bfloat16)}


def expand_rows(per_degree):
    return jnp.concatenate([jnp.broadcast_to(per_degree[degree:degree + 1], (2 * degree + 1,) + per_degree.shape[1:]) for degree in range(per_degree.shape[0])], axis=0)


def block_forward(x_blk, norm_gain, up_f, gate_f, down_f, grid_in, grid_back):
    x_f = x_blk.astype(jnp.float32)
    scalar = x_f[:, 0, :]
    mean_s = jnp.mean(scalar, axis=-1, keepdims=True)
    centered = scalar - mean_s
    var_s = jnp.mean(centered * centered, axis=-1, keepdims=True)
    vector = x_f[:, 1:, :]
    mean_sq = jnp.mean(vector * vector, axis=(1, 2), keepdims=True)
    normed = jnp.concatenate([(centered * lax.rsqrt(var_s + NORM_EPS))[:, None, :], vector * lax.rsqrt(mean_sq + NORM_EPS)], axis=1)
    normed = (normed * expand_rows(norm_gain)).astype(jnp.bfloat16).astype(jnp.float32)
    hidden_act = jnp.einsum('nkc,kch->nkh', normed, expand_rows(up_f)).astype(jnp.bfloat16).astype(jnp.float32)
    pre_gate = jnp.einsum('nc,ch->nh', normed[:, 0, :], gate_f).astype(jnp.bfloat16).astype(jnp.float32)
    gate_val = jax.nn.silu(pre_gate).astype(jnp.bfloat16)
    pre_grid = jnp.einsum('nkh,kg->ngh', hidden_act, grid_in).astype(jnp.bfloat16).astype(jnp.float32)
    grid_val = jax.nn.silu(pre_grid).astype(jnp.bfloat16).astype(jnp.float32)
    back_proj = jnp.einsum('ngh,gk->nkh', grid_val, grid_back).astype(jnp.bfloat16)
    mixed_act = jnp.concatenate([gate_val[:, None, :], back_proj], axis=1).astype(jnp.float32)
    ffn_delta = jnp.einsum('nkh,khc->nkc', mixed_act, expand_rows(down_f))
    return (x_f + ffn_delta).astype(jnp.bfloat16)


def reference(irreps, norm_gain, w_up, w_gate, w_down, to_grid, from_grid, grad_out):
    up_f = w_up.astype(jnp.float32)
    gate_f = w_gate.astype(jnp.float32)
    down_f = w_down.astype(jnp.float32)
    grid_in = to_grid.astype(jnp.bfloat16).astype(jnp.float32)
    grid_back = from_grid.astype(jnp.bfloat16).astype(jnp.float32)
    blk_count = N_NODES // ROW_BLOCK
    x_blocks = irreps.reshape(blk_count, ROW_BLOCK, COEFS, CHANNELS)
    g_blocks = grad_out.reshape(blk_count, ROW_BLOCK, COEFS, CHANNELS)

    def scan_step(grad_sums, blk_pair):
        def local_fn(x_in, up_in, gate_in, down_in):
            return block_forward(x_in, norm_gain, up_in, gate_in, down_in, grid_in, grid_back)
        out_blk, pull_back = jax.vjp(local_fn, blk_pair[0], up_f, gate_f, down_f)
        dx_blk, d_up, d_gate, d_down = pull_back(blk_pair[1])
        new_sums = (grad_sums[0] + d_up, grad_sums[1] + d_gate, grad_sums[2] + d_down)
        return new_sums, (out_blk, dx_blk)

    init_sums = (jnp.zeros_like(up_f), jnp.zeros_like(gate_f), jnp.zeros_like(down_f))
    total_sums, (out_blocks, dx_blocks) = lax.scan(scan_step, init_sums, (x_blocks, g_blocks))
    out_irreps = out_blocks.reshape(N_NODES, COEFS, CHANNELS)
    d_irreps = dx_blocks.reshape(N_NODES, COEFS, CHANNELS)
    return (out_irreps, d_irreps, total_sums[0].astype(jnp.bfloat16), total_sums[1].astype(jnp.bfloat16), total_sums[2].astype(jnp.bfloat16))
```

```python
import jax
import jax.numpy as jnp
from jax import lax
from jax.experimental import pallas as pl
from jax.experimental.pallas import tpu as pltpu
from jax.sharding import PartitionSpec as P

NORM_EPS = 1e-5
F32 = jnp.float32
BF16 = jnp.bfloat16
MESH = pl.DeviceIdType.MESH
LANES = 128
STEP = 56


def degree_of(coef):
    total = (coef >= 1).astype(jnp.int32)
    for deg in range(2, 7):
        total = total + (coef >= deg * deg).astype(jnp.int32)
    return total


def mm(lhs, rhs):
    return jnp.dot(lhs, rhs, preferred_element_type=F32)


def mm_nt(lhs, rhs):
    return lax.dot_general(lhs, rhs, (((1,), (1,)), ((), ())), preferred_element_type=F32)


def sigmoid(val):
    return 0.5 * jnp.tanh(0.5 * val) + 0.5


def fused_kernel(x_hbm, g_hbm, up_hbm, gate_hbm, down_hbm, gain_hbm, tt_ref, t_ref, f_ref, ft_ref,
                 out_hbm, dx_hbm, gup_ref, ggate_ref, gdown_ref,
                 x_buf, g_buf, o_buf, n_buf, dn_buf, y0, y1, z0, z1,
                 wu, wg, wd, gain_in, wut, wgt, wdt, gain_b,
                 w_send, w_recv, w_loc, in_send, in_recv, in_loc, o_send, o_recv, o_loc):
    chunks, coefs = x_buf.shape[0], x_buf.shape[1]
    share = x_hbm.shape[1]
    own = chunks * LANES
    me = lax.axis_index('tp')
    mate = me ^ 1

    def rows(who, size):
        return pl.ds(pl.multiple_of(who * size, size), size)

    def lanes(who, chunk):
        return pl.ds(pl.multiple_of(who * own + chunk * LANES, LANES), LANES)

    barrier = pltpu.get_barrier_semaphore()
    for flip in (1, 2, 3):
        pl.semaphore_signal(barrier, inc=1, device_id={'tp': me ^ flip}, device_id_type=MESH)
    pl.semaphore_wait(barrier, 3)

    def weight_parts(who):
        hid = up_hbm.shape[1]
        return (wu.at[:, rows(who, hid), :], wd.at[:, rows(who, hid), :], wg.at[rows(who, hid), :], gain_in.at[who])

    sources = (up_hbm, down_hbm, gate_hbm, gain_hbm)

    def weight_copies(flip):
        if flip == 3:
            parts = weight_parts(me ^ 2)
            pairs = zip(parts, parts)
            peer = mate
        else:
            pairs = zip(sources, weight_parts(me))
            peer = me ^ flip
        return [pltpu.make_async_remote_copy(src, dst, w_send.at[flip, i], w_recv.at[flip, i], device_id={'tp': peer}, device_id_type=MESH)
                for i, (src, dst) in enumerate(pairs)]

    own_weights = [pltpu.make_async_copy(src, dst, w_loc.at[i]) for i, (src, dst) in enumerate(zip(sources, weight_parts(me)))]
    far_weights, mate_weights, relay_weights = weight_copies(2), weight_copies(1), weight_copies(3)
    for copy in far_weights + mate_weights + own_weights:
        copy.start()

    def input_copy(tensor, chunk, flip):
        src, buf = ((x_hbm, x_buf), (g_hbm, g_buf))[tensor]
        return pltpu.make_async_remote_copy(
            src.at[:, :, lanes(me ^ flip, chunk)], buf.at[chunk, :, rows(me, share), :],
            in_send.at[tensor, chunk, flip], in_recv.at[tensor, chunk, flip],
            device_id={'tp': me ^ flip}, device_id_type=MESH)

    def input_local(tensor, chunk):
        src, buf = ((x_hbm, x_buf), (g_hbm, g_buf))[tensor]
        return pltpu.make_async_copy(src.at[:, :, lanes(me, chunk)], buf.at[chunk, :, rows(me, share), :], in_loc.at[tensor, chunk])

    def output_copy(tensor, chunk, flip):
        buf, dst = ((o_buf, out_hbm), (g_buf, dx_hbm))[tensor]
        return pltpu.make_async_remote_copy(
            buf.at[chunk, :, rows(me ^ flip, share), :], dst.at[:, :, lanes(me, chunk)],
            o_send.at[tensor, chunk, flip], o_recv.at[tensor, chunk, flip],
            device_id={'tp': me ^ flip}, device_id_type=MESH)

    def output_local(tensor, chunk):
        buf, dst = ((o_buf, out_hbm), (g_buf, dx_hbm))[tensor]
        return pltpu.make_async_copy(buf.at[chunk, :, rows(me, share), :], dst.at[:, :, lanes(me, chunk)], o_loc.at[tensor, chunk])

    def start_inputs(chunk, carry):
        for flip in (2, 3, 1):
            for tensor in (0, 1):
                input_copy(tensor, chunk, flip).start()
        for tensor in (0, 1):
            input_local(tensor, chunk).start()
        return carry

    lax.fori_loop(0, chunks, start_inputs, 0)

    gup_ref[...] = jnp.zeros_like(gup_ref)
    ggate_ref[...] = jnp.zeros_like(ggate_ref)
    gdown_ref[...] = jnp.zeros_like(gdown_ref)
    blank = jnp.zeros((LANES, LANES), F32)
    for pad in range(coefs, STEP):
        for ref in (y0, y1, z0, z1):
            ref[pl.ds(pad, LANES, stride=STEP), :] = blank
    for ref in (z0, z1):
        ref[pl.ds(0, LANES, stride=STEP), :] = blank

    for far, relay in zip(far_weights, relay_weights):
        far.wait_recv()
        relay.start()
    for copy in far_weights:
        copy.wait_send()
    for copy in mate_weights + relay_weights + own_weights:
        copy.wait()

    def turn(deg, carry):
        wut[deg] = wu[deg].astype(F32).T.astype(BF16)
        wdt[deg] = wd[deg].astype(F32).T.astype(BF16)
        return carry

    degrees = wu.shape[0]
    lax.fori_loop(0, degrees, turn, 0)
    wgt[...] = wg[...].astype(F32).T.astype(BF16)
    gains = jnp.concatenate([gain_in[i][:, :share] for i in range(gain_in.shape[0])], axis=1)
    gains = jnp.concatenate([gains] * (LANES // gains.shape[0]), axis=0).T
    for deg in range(degrees):
        gain_b[deg] = jnp.broadcast_to(gains[:, deg:deg + 1], (LANES, LANES))

    inv_chan = 1.0 / LANES
    inv_vec = 1.0 / (LANES * (coefs - 1))

    def chunk_step(chunk, carry):
        for flip in (2, 3, 1):
            for tensor in (0, 1):
                input_copy(tensor, chunk, flip).wait_recv()
        for tensor in (0, 1):
            input_local(tensor, chunk).wait()

        def square_sum(k, acc):
            val = x_buf[chunk, k].astype(F32)
            return acc + val * val

        sq = lax.fori_loop(1, coefs, square_sum, jnp.zeros((LANES, LANES), F32), unroll=8)
        inv_v = lax.rsqrt(jnp.sum(sq, axis=0, keepdims=True) * inv_vec + NORM_EPS)
        scalar = x_buf[chunk, 0].astype(F32)
        cent = scalar - jnp.sum(scalar, axis=0, keepdims=True) * inv_chan
        inv_s = lax.rsqrt(jnp.sum(cent * cent, axis=0, keepdims=True) * inv_chan + NORM_EPS)
        hat_s = cent * inv_s
        n_zero = (hat_s * gain_b[0]).astype(BF16)
        n_buf[0] = n_zero
        y_zero = mm(wu[0], n_zero)
        y0[pl.ds(0, LANES, stride=STEP), :] = y_zero[:LANES]
        y1[pl.ds(0, LANES, stride=STEP), :] = y_zero[LANES:]

        def up_step(k, carry):
            deg = degree_of(k)
            n_k = (x_buf[chunk, k].astype(F32) * inv_v * gain_b[deg]).astype(BF16)
            n_buf[k] = n_k
            y_k = mm(wu[deg], n_k)
            y0[pl.ds(k, LANES, stride=STEP), :] = y_k[:LANES]
            y1[pl.ds(k, LANES, stride=STEP), :] = y_k[LANES:]
            dm_k = mm(wd[deg], g_buf[chunk, k])
            z0[pl.ds(k, LANES, stride=STEP), :] = dm_k[:LANES]
            z1[pl.ds(k, LANES, stride=STEP), :] = dm_k[LANES:]
            return carry

        lax.fori_loop(1, coefs, up_step, 0, unroll=4)

        def grid_step(j, carry):
            span = pl.ds(pl.multiple_of(j * STEP, 8), STEP)
            y_j = jnp.concatenate([y0[span, :], y1[span, :]], axis=1).astype(BF16)
            dm_j = jnp.concatenate([z0[span, :], z1[span, :]], axis=1).astype(BF16)
            u = mm(tt_ref[...], y_j).astype(BF16).astype(F32)
            sig = sigmoid(u)
            act = u * sig
            z_j = mm(ft_ref[...], act.astype(BF16))
            z0[span, :] = z_j[:, :LANES]
            z1[span, :] = z_j[:, LANES:]
            ds = mm(f_ref[...], dm_j).astype(BF16).astype(F32)
            du = (ds * (sig + act * (1.0 - sig))).astype(BF16)
            dy_j = mm(t_ref[...], du)
            y0[span, :] = dy_j[:, :LANES]
            y1[span, :] = dy_j[:, LANES:]
            return carry

        lax.fori_loop(0, LANES, grid_step, 0, unroll=2)

        def hidden_grad(k):
            picked = pl.ds(k, LANES, stride=STEP)
            return jnp.concatenate([y0[picked, :], y1[picked, :]], axis=0).astype(BF16)

        g_zero = g_buf[chunk, 0]
        n_zero = n_buf[0]
        pre = mm(wg[...], n_zero).astype(BF16).astype(F32)
        sig = sigmoid(pre)
        gate = pre * sig
        dm_zero = mm(wd[0], g_zero).astype(BF16).astype(F32)
        d_pre = (dm_zero * (sig + gate * (1.0 - sig))).astype(BF16)
        gate = gate.astype(BF16)
        o_buf[chunk, 0] = (x_buf[chunk, 0].astype(F32) + mm(wdt[0], gate)).astype(BF16)
        gdown_ref[0] += mm_nt(gate, g_zero)
        dy_zero = hidden_grad(0)
        gup_ref[0] += mm_nt(dy_zero, n_zero)
        ggate_ref[...] += mm_nt(d_pre, n_zero)
        dn_zero = (mm(wut[0], dy_zero) + mm(wgt[...], d_pre)).astype(BF16).astype(F32)

        def down_step(k, acc):
            deg = degree_of(k)
            picked = pl.ds(k, LANES, stride=STEP)
            m_k = jnp.concatenate([z0[picked, :], z1[picked, :]], axis=0).astype(BF16)
            dy_k = hidden_grad(k)
            x_k = x_buf[chunk, k].astype(F32)
            o_buf[chunk, k] = (x_k + mm(wdt[deg], m_k)).astype(BF16)
            gdown_ref[deg] += mm_nt(m_k, g_buf[chunk, k])
            dn_k = mm(wut[deg], dy_k).astype(BF16)
            dn_buf[k] = dn_k
            gup_ref[deg] += mm_nt(dy_k, n_buf[k])
            return acc + dn_k.astype(F32) * gain_b[deg] * x_k

        dot_v = lax.fori_loop(1, coefs, down_step, jnp.zeros((LANES, LANES), F32), unroll=4)
        for flip in (2, 3, 1):
            output_copy(0, chunk, flip).start()
        output_local(0, chunk).start()

        z0[pl.ds(0, LANES, stride=STEP), :] = blank
        z1[pl.ds(0, LANES, stride=STEP), :] = blank
        dh_s = dn_zero * gain_b[0]
        mean_d = jnp.sum(dh_s, axis=0, keepdims=True) * inv_chan
        mean_dx = jnp.sum(dh_s * hat_s, axis=0, keepdims=True) * inv_chan
        dx_s = inv_s * (dh_s - mean_d - hat_s * mean_dx)
        g_buf[chunk, 0] = (dx_s + g_zero.astype(F32)).astype(BF16)
        coef_v = inv_v * inv_v * inv_v * (jnp.sum(dot_v, axis=0, keepdims=True) * inv_vec)

        def back_step(k, carry):
            dh = dn_buf[k].astype(F32) * gain_b[degree_of(k)]
            dx = inv_v * dh - x_buf[chunk, k].astype(F32) * coef_v
            g_buf[chunk, k] = (dx + g_buf[chunk, k].astype(F32)).astype(BF16)
            return carry

        lax.fori_loop(1, coefs, back_step, 0, unroll=4)
        for flip in (2, 3, 1):
            output_copy(1, chunk, flip).start()
        output_local(1, chunk).start()
        return carry

    lax.fori_loop(0, chunks, chunk_step, 0)

    def finish(chunk, carry):
        for tensor in (0, 1):
            for flip in (2, 3, 1):
                input_copy(tensor, chunk, flip).wait_send()
                output_copy(tensor, chunk, flip).wait()
            output_local(tensor, chunk).wait()
        return carry

    lax.fori_loop(0, chunks, finish, 0)


def solution(mesh):
    tp_size = mesh.shape['tp']
    act_spec = P('dp', None, 'tp')
    in_specs = (act_spec, P(None, 'tp'), P(None, None, 'tp'), P(None, 'tp'), P(None, 'tp', None), P(None, None), P(None, None), act_spec)
    out_specs = (act_spec, act_spec, P(None, None, 'tp'), P(None, 'tp'), P(None, 'tp', None))

    def local_step(x_loc, gain_loc, up_loc, gate_loc, down_loc, to_grid, from_grid, grad_loc):
        nodes, coefs, share = x_loc.shape
        degrees, channels, hid = up_loc.shape
        hidden = hid * tp_size
        points = to_grid.shape[1]
        pts = -(-points // 8) * 8
        chunks = nodes // tp_size // LANES
        x_t = jnp.transpose(x_loc, (1, 2, 0))
        g_t = jnp.transpose(grad_loc, (1, 2, 0))
        up_t = jnp.transpose(up_loc, (0, 2, 1))
        gate_t = jnp.transpose(gate_loc, (1, 0))
        gain_pad = jnp.pad(gain_loc, ((0, 8 - degrees), (0, LANES - share)))
        t_pad = jnp.pad(to_grid.astype(BF16), ((0, STEP - coefs), (0, pts - points)))
        f_pad = jnp.pad(from_grid.astype(BF16), ((0, pts - points), (1, STEP - coefs)))
        hbm = pl.BlockSpec(memory_space=pl.ANY)
        vmem = pl.BlockSpec(memory_space=pltpu.VMEM)
        dma = pltpu.SemaphoreType.DMA
        act = (chunks, coefs, channels, LANES)
        wide = pltpu.VMEM((LANES * STEP, LANES), F32)
        out_t, dx_t, g_up, g_gate, g_down = pl.pallas_call(
            fused_kernel,
            out_shape=(
                jax.ShapeDtypeStruct(x_t.shape, BF16),
                jax.ShapeDtypeStruct(x_t.shape, BF16),
                jax.ShapeDtypeStruct((degrees, hidden, channels), F32),
                jax.ShapeDtypeStruct((hidden, channels), F32),
                jax.ShapeDtypeStruct((degrees, hidden, channels), F32)),
            in_specs=[hbm] * 6 + [vmem] * 4,
            out_specs=(hbm, hbm, vmem, vmem, vmem),
            scratch_shapes=[
                pltpu.VMEM(act, BF16), pltpu.VMEM(act, BF16), pltpu.VMEM(act, BF16),
                pltpu.VMEM(act[1:], BF16), pltpu.VMEM(act[1:], BF16),
                wide, wide, wide, wide,
                pltpu.VMEM((degrees, hidden, channels), BF16), pltpu.VMEM((hidden, channels), BF16),
                pltpu.VMEM((degrees, hidden, channels), BF16), pltpu.VMEM((tp_size, 8, LANES), F32),
                pltpu.VMEM((degrees, channels, hidden), BF16), pltpu.VMEM((channels, hidden), BF16),
                pltpu.VMEM((degrees, channels, hidden), BF16), pltpu.VMEM((degrees, channels, LANES), F32),
                dma((4, 4)), dma((4, 4)), dma((4,)),
                dma((2, chunks, 4)), dma((2, chunks, 4)), dma((2, chunks)),
                dma((2, chunks, 4)), dma((2, chunks, 4)), dma((2, chunks))],
            compiler_params=pltpu.CompilerParams(collective_id=0, has_side_effects=True, vmem_limit_bytes=62 * 1024 * 1024),
            name='fused',
        )(x_t, g_t, up_t, gate_t, down_loc, gain_pad, t_pad.T, t_pad, f_pad, f_pad.T)
        back = lambda val: jnp.transpose(val, (2, 0, 1))

        def reduce(val, dim):
            return lax.psum(lax.psum_scatter(val, 'tp', scatter_dimension=dim, tiled=True), 'dp').astype(BF16)

        d_up = jnp.transpose(reduce(g_up, 1), (0, 2, 1))
        d_gate = jnp.transpose(reduce(g_gate, 0), (1, 0))
        return back(out_t), back(dx_t), d_up, d_gate, reduce(g_down, 1)

    return jax.shard_map(local_step, mesh=mesh, in_specs=in_specs, out_specs=out_specs, check_vma=False)
```

```python
import jax
import jax.numpy as jnp
from jax import lax
from jax.experimental import pallas as pl
from jax.experimental.pallas import tpu as pltpu
from jax.sharding import PartitionSpec as P

NORM_EPS = 1e-5
F32 = jnp.float32
BF16 = jnp.bfloat16
MESH = pl.DeviceIdType.MESH
LANES = 128
STEP = 56
WIDE = 4


def degree_of(coef):
    total = (coef >= 1).astype(jnp.int32)
    for deg in range(2, 7):
        total = total + (coef >= deg * deg).astype(jnp.int32)
    return total


def mm(lhs, rhs):
    return jnp.dot(lhs, rhs, preferred_element_type=F32)


def mm_nt(lhs, rhs):
    return lax.dot_general(lhs, rhs, (((1,), (1,)), ((), ())), preferred_element_type=F32)


def sigmoid(val):
    return 0.5 * jnp.tanh(0.5 * val) + 0.5


def fused_kernel(x_hbm, g_hbm, up_hbm, gate_hbm, down_hbm, gain_hbm, tg_ref, fg_ref,
                 out_hbm, dx_hbm, dup_ref, dgate_ref, ddown_ref,
                 x_buf, g_buf, o_buf, n_buf, dn_buf, y0, y1, z0, z1,
                 wu, wg, wd, gain_in, wut, wgt, wdt, gain_b,
                 tt_ref, t_ref, f_ref, ft_ref, pad_buf, u_buf, s_buf, act_buf, du_buf,
                 g_sum, half_buf, mate_buf, far_buf, fin_buf,
                 w_send, w_recv, w_loc, in_send, in_recv, in_loc, o_send, o_recv, o_loc, r_send, r_recv):
    chunks, coefs = x_buf.shape[0], x_buf.shape[1]
    share = x_hbm.shape[1]
    own = chunks * LANES
    me = lax.axis_index('tp')
    mate = me ^ 1
    side = lax.axis_index('dp')

    def rows(who, size):
        return pl.ds(pl.multiple_of(who * size, size), size)

    def lanes(who, chunk):
        return pl.ds(pl.multiple_of(who * own + chunk * LANES, LANES), LANES)

    barrier = pltpu.get_barrier_semaphore()
    for flip in (1, 2, 3):
        pl.semaphore_signal(barrier, inc=1, device_id={'tp': me ^ flip}, device_id_type=MESH)
    pl.semaphore_signal(barrier, inc=1, device_id={'dp': 1 - side}, device_id_type=MESH)
    pl.semaphore_wait(barrier, 4)

    def weight_parts(who):
        hid = up_hbm.shape[1]
        return (wu.at[:, rows(who, hid), :], wd.at[:, rows(who, hid), :], wg.at[rows(who, hid), :], gain_in.at[who])

    sources = (up_hbm, down_hbm, gate_hbm, gain_hbm)

    def weight_copies(flip):
        if flip == 3:
            parts = weight_parts(me ^ 2)
            pairs = zip(parts, parts)
            peer = mate
        else:
            pairs = zip(sources, weight_parts(me))
            peer = me ^ flip
        return [pltpu.make_async_remote_copy(src, dst, w_send.at[flip, i], w_recv.at[flip, i], device_id={'tp': peer}, device_id_type=MESH)
                for i, (src, dst) in enumerate(pairs)]

    own_weights = [pltpu.make_async_copy(src, dst, w_loc.at[i]) for i, (src, dst) in enumerate(zip(sources, weight_parts(me)))]
    far_weights, mate_weights, relay_weights = weight_copies(2), weight_copies(1), weight_copies(3)
    for copy in far_weights + mate_weights + own_weights:
        copy.start()

    def input_copy(tensor, chunk, flip):
        src, buf = ((x_hbm, x_buf), (g_hbm, g_buf))[tensor]
        return pltpu.make_async_remote_copy(
            src.at[:, :, lanes(me ^ flip, chunk)], buf.at[chunk, :, rows(me, share), :],
            in_send.at[tensor, chunk, flip], in_recv.at[tensor, chunk, flip],
            device_id={'tp': me ^ flip}, device_id_type=MESH)

    def input_local(tensor, chunk):
        src, buf = ((x_hbm, x_buf), (g_hbm, g_buf))[tensor]
        return pltpu.make_async_copy(src.at[:, :, lanes(me, chunk)], buf.at[chunk, :, rows(me, share), :], in_loc.at[tensor, chunk])

    def output_copy(tensor, chunk, flip):
        buf, dst = ((o_buf, out_hbm), (g_buf, dx_hbm))[tensor]
        return pltpu.make_async_remote_copy(
            buf.at[chunk, :, rows(me ^ flip, share), :], dst.at[:, :, lanes(me, chunk)],
            o_send.at[tensor, chunk, flip], o_recv.at[tensor, chunk, flip],
            device_id={'tp': me ^ flip}, device_id_type=MESH)

    def output_local(tensor, chunk):
        buf, dst = ((o_buf, out_hbm), (g_buf, dx_hbm))[tensor]
        return pltpu.make_async_copy(buf.at[chunk, :, rows(me, share), :], dst.at[:, :, lanes(me, chunk)], o_loc.at[tensor, chunk])

    def start_outputs(tensor, chunk):
        @pl.when(chunk < chunks - 1)
        def _():
            for flip in (2, 3):
                output_copy(tensor, chunk, flip).start()

        output_copy(tensor, chunk, 1).start()
        output_local(tensor, chunk).start()

    def start_inputs(chunk, carry):
        for flip in (2, 3, 1):
            for tensor in (0, 1):
                input_copy(tensor, chunk, flip).start()
        for tensor in (0, 1):
            input_local(tensor, chunk).start()
        return carry

    lax.fori_loop(0, chunks, start_inputs, 0)

    g_sum[...] = jnp.zeros_like(g_sum)
    blank = jnp.zeros((LANES, LANES), F32)
    for pad in range(coefs, STEP):
        for ref in (y0, y1, z0, z1):
            ref[pl.ds(pad, LANES, stride=STEP), :] = blank
    for ref in (z0, z1):
        ref[pl.ds(0, LANES, stride=STEP), :] = blank

    points = tg_ref.shape[1]
    pts = t_ref.shape[1]
    pad_buf[...] = jnp.zeros_like(pad_buf)
    pad_buf[:coefs, :points] = tg_ref[...].astype(BF16).astype(F32)
    t_ref[...] = pad_buf[:STEP, :pts].astype(BF16)
    tt_ref[...] = (0.5 * pad_buf[...]).T[:pts, :STEP].astype(BF16)
    pad_buf[...] = jnp.zeros_like(pad_buf)
    pad_buf[1:coefs, :points] = fg_ref[...].astype(BF16).astype(F32)
    ft_ref[...] = pad_buf[:STEP, :pts].astype(BF16)
    f_ref[...] = (0.5 * pad_buf[...]).T[:pts, :STEP].astype(BF16)

    for far, relay in zip(far_weights, relay_weights):
        far.wait_recv()
        relay.start()
    for copy in far_weights:
        copy.wait_send()
    for copy in mate_weights + relay_weights + own_weights:
        copy.wait()

    def turn(deg, carry):
        wut[deg] = wu[deg].astype(F32).T.astype(BF16)
        wdt[deg] = wd[deg].astype(F32).T.astype(BF16)
        return carry

    degrees = wu.shape[0]
    lax.fori_loop(0, degrees, turn, 0)
    wgt[...] = wg[...].astype(F32).T.astype(BF16)
    gains = jnp.concatenate([gain_in[i] for i in range(gain_in.shape[0])], axis=1)
    pad_buf[:degrees, :LANES] = gains
    gains = pad_buf[:, :LANES].T
    for deg in range(degrees):
        gain_b[deg] = jnp.broadcast_to(gains[:, deg:deg + 1], (LANES, LANES))

    inv_chan = 1.0 / LANES
    inv_vec = 1.0 / (LANES * (coefs - 1))

    def chunk_step(chunk, carry):
        for flip in (2, 3, 1):
            for tensor in (0, 1):
                input_copy(tensor, chunk, flip).wait_recv()
        for tensor in (0, 1):
            input_local(tensor, chunk).wait()

        def square_sum(k, acc):
            val = x_buf[chunk, k].astype(F32)
            return acc + val * val

        sq = lax.fori_loop(1, coefs, square_sum, jnp.zeros((LANES, LANES), F32), unroll=8)
        inv_v = lax.rsqrt(jnp.sum(sq, axis=0, keepdims=True) * inv_vec + NORM_EPS)
        scalar = x_buf[chunk, 0].astype(F32)
        cent = scalar - jnp.sum(scalar, axis=0, keepdims=True) * inv_chan
        inv_s = lax.rsqrt(jnp.sum(cent * cent, axis=0, keepdims=True) * inv_chan + NORM_EPS)
        hat_s = cent * inv_s
        n_zero = (hat_s * gain_b[0]).astype(BF16)
        n_buf[0] = n_zero
        y_zero = mm(wu[0], n_zero)
        y0[pl.ds(0, LANES, stride=STEP), :] = y_zero[:LANES]
        y1[pl.ds(0, LANES, stride=STEP), :] = y_zero[LANES:]

        def up_step(k, carry):
            deg = degree_of(k)
            n_k = (x_buf[chunk, k].astype(F32) * inv_v * gain_b[deg]).astype(BF16)
            n_buf[k] = n_k
            y_k = mm(wu[deg], n_k)
            y0[pl.ds(k, LANES, stride=STEP), :] = y_k[:LANES]
            y1[pl.ds(k, LANES, stride=STEP), :] = y_k[LANES:]
            dm_k = mm(wd[deg], g_buf[chunk, k])
            z0[pl.ds(k, LANES, stride=STEP), :] = dm_k[:LANES]
            z1[pl.ds(k, LANES, stride=STEP), :] = dm_k[LANES:]
            return carry

        lax.fori_loop(1, coefs, up_step, 0, unroll=4)

        groups = LANES // WIDE

        def spans_of(group):
            return [pl.ds(pl.multiple_of((group * WIDE + i) * STEP, 8), STEP) for i in range(WIDE)]

        def grid_step(i, carry):
            late = spans_of(jnp.maximum(i - 2, 0))
            early = spans_of(jnp.minimum(i, groups - 1))
            ys = [jnp.concatenate([y0[span, :], y1[span, :]], axis=1).astype(BF16) for span in early]
            dms = [jnp.concatenate([z0[span, :], z1[span, :]], axis=1).astype(BF16) for span in early]
            zs = [mm(ft_ref[...], act_buf[n]) for n in range(WIDE)]
            dys = [mm(t_ref[...], du_buf[n]) for n in range(WIDE)]
            for n in range(WIDE):
                half = u_buf[n].astype(F32)
                tan = jnp.tanh(half)
                both = half * tan
                act_buf[n] = (half + both).astype(BF16)
                du_buf[n] = (s_buf[n].astype(F32) * ((1.0 + tan) + (half - both * tan))).astype(BF16)
            for n in range(WIDE):
                u_buf[n] = mm(tt_ref[...], ys[n]).astype(BF16)
                s_buf[n] = mm(f_ref[...], dms[n]).astype(BF16)
            for span, z_j, dy_j in zip(late, zs, dys):
                z0[span, :] = z_j[:, :LANES]
                z1[span, :] = z_j[:, LANES:]
                y0[span, :] = dy_j[:, :LANES]
                y1[span, :] = dy_j[:, LANES:]
            return carry

        lax.fori_loop(0, groups + 2, grid_step, 0)

        def hidden_grad(k):
            picked = pl.ds(k, LANES, stride=STEP)
            return jnp.concatenate([y0[picked, :], y1[picked, :]], axis=0).astype(BF16)

        g_zero = g_buf[chunk, 0]
        n_zero = n_buf[0]
        pre = mm(wg[...], n_zero).astype(BF16).astype(F32)
        sig = sigmoid(pre)
        gate = pre * sig
        dm_zero = mm(wd[0], g_zero).astype(BF16).astype(F32)
        d_pre = (dm_zero * (sig + gate * (1.0 - sig))).astype(BF16)
        gate = gate.astype(BF16)
        o_buf[chunk, 0] = (x_buf[chunk, 0].astype(F32) + mm(wdt[0], gate)).astype(BF16)
        g_sum[degrees] += mm_nt(gate, g_zero)
        dy_zero = hidden_grad(0)
        g_sum[0] += mm_nt(dy_zero, n_zero)
        g_sum[2 * degrees] += mm_nt(d_pre, n_zero)
        dn_zero = (mm(wut[0], dy_zero) + mm(wgt[...], d_pre)).astype(BF16).astype(F32)

        def down_step(k, acc):
            deg = degree_of(k)
            picked = pl.ds(k, LANES, stride=STEP)
            m_k = jnp.concatenate([z0[picked, :], z1[picked, :]], axis=0).astype(BF16)
            dy_k = hidden_grad(k)
            x_k = x_buf[chunk, k].astype(F32)
            o_buf[chunk, k] = (x_k + mm(wdt[deg], m_k)).astype(BF16)
            g_sum[degrees + deg] += mm_nt(m_k, g_buf[chunk, k])
            dn_k = mm(wut[deg], dy_k).astype(BF16)
            dn_buf[k] = dn_k
            g_sum[deg] += mm_nt(dy_k, n_buf[k])
            return acc + dn_k.astype(F32) * gain_b[deg] * x_k

        dot_v = lax.fori_loop(1, coefs, down_step, jnp.zeros((LANES, LANES), F32), unroll=4)
        start_outputs(0, chunk)

        z0[pl.ds(0, LANES, stride=STEP), :] = blank
        z1[pl.ds(0, LANES, stride=STEP), :] = blank
        dh_s = dn_zero * gain_b[0]
        mean_d = jnp.sum(dh_s, axis=0, keepdims=True) * inv_chan
        mean_dx = jnp.sum(dh_s * hat_s, axis=0, keepdims=True) * inv_chan
        dx_s = inv_s * (dh_s - mean_d - hat_s * mean_dx)
        g_buf[chunk, 0] = (dx_s + g_zero.astype(F32)).astype(BF16)
        coef_v = inv_v * inv_v * inv_v * (jnp.sum(dot_v, axis=0, keepdims=True) * inv_vec)

        def back_step(k, carry):
            dh = dn_buf[k].astype(F32) * gain_b[degree_of(k)]
            dx = inv_v * dh - x_buf[chunk, k].astype(F32) * coef_v
            g_buf[chunk, k] = (dx + g_buf[chunk, k].astype(F32)).astype(BF16)
            return carry

        lax.fori_loop(1, coefs, back_step, 0, unroll=4)
        start_outputs(1, chunk)
        return carry

    lax.fori_loop(0, chunks, chunk_step, 0)

    hid = up_hbm.shape[1]
    part = hid // 2
    slices = half_buf.shape[0]

    def sum_rows(who, where):
        return pl.ds(pl.multiple_of(who * hid + where * part, part), part)

    def push(src, dst, num, peer):
        return pltpu.make_async_remote_copy(src, dst, r_send.at[num], r_recv.at[num], device_id=peer, device_id_type=MESH)

    halves = [push(g_sum.at[:, sum_rows(n, 1 - side), :], half_buf.at[n], n, {'dp': 1 - side}) for n in range(slices)]
    for copy in halves:
        copy.start()
    for copy in halves:
        copy.wait_recv()
    rows_all = g_sum.shape[0]

    def add_half(row, carry):
        for n in range(slices):
            half_buf[n, row] += g_sum[row, sum_rows(n, side), :]
        return carry

    lax.fori_loop(0, rows_all, add_half, 0)
    shares = [push(half_buf.at[mate], mate_buf.at[0], slices, {'tp': mate}),
              push(half_buf.at[mate ^ 2], mate_buf.at[1], slices + 1, {'tp': mate})]
    for copy in shares:
        copy.start()
    for copy in shares:
        copy.wait()

    def add_mate(row, carry):
        mate_buf[0, row] += half_buf[me, row]
        mate_buf[1, row] += half_buf[me ^ 2, row]
        return carry

    lax.fori_loop(0, rows_all, add_mate, 0)
    cross = push(mate_buf.at[1], far_buf, slices + 2, {'tp': me ^ 2})
    cross.start()
    for tensor in (0, 1):
        for flip in (2, 3):
            output_copy(tensor, chunks - 1, flip).start()
    cross.wait()
    mine = pl.ds(pl.multiple_of(side * part, part), part)

    def add_far(row, carry):
        fin_buf[row, mine, :] = (mate_buf[0, row] + far_buf[row]).astype(BF16)
        return carry

    lax.fori_loop(0, rows_all, add_far, 0)
    last = push(fin_buf.at[:, mine, :], fin_buf.at[:, mine, :], slices + 3, {'dp': 1 - side})
    last.start()
    last.wait()
    for copy in halves:
        copy.wait_send()
    dup_ref[...] = fin_buf[:degrees]
    ddown_ref[...] = fin_buf[degrees:2 * degrees]
    dgate_ref[...] = fin_buf[2 * degrees]

    def finish(chunk, carry):
        for tensor in (0, 1):
            for flip in (2, 3, 1):
                input_copy(tensor, chunk, flip).wait_send()
                output_copy(tensor, chunk, flip).wait()
            output_local(tensor, chunk).wait()
        return carry

    lax.fori_loop(0, chunks, finish, 0)


def solution(mesh):
    tp_size = mesh.shape['tp']
    act_spec = P('dp', None, 'tp')
    in_specs = (act_spec, P(None, 'tp'), P(None, None, 'tp'), P(None, 'tp'), P(None, 'tp', None), P(None, None), P(None, None), act_spec)
    out_specs = (act_spec, act_spec, P(None, None, 'tp'), P(None, 'tp'), P(None, 'tp', None))

    def local_step(x_loc, gain_loc, up_loc, gate_loc, down_loc, to_grid, from_grid, grad_loc):
        nodes, coefs, share = x_loc.shape
        degrees, channels, hid = up_loc.shape
        hidden = hid * tp_size
        points = to_grid.shape[1]
        pts = -(-points // 8) * 8
        chunks = nodes // tp_size // LANES
        x_t = jnp.transpose(x_loc, (1, 2, 0))
        g_t = jnp.transpose(grad_loc, (1, 2, 0))
        up_t = jnp.transpose(up_loc, (0, 2, 1))
        gate_t = jnp.transpose(gate_loc, (1, 0))
        hbm = pl.BlockSpec(memory_space=pl.ANY)
        vmem = pl.BlockSpec(memory_space=pltpu.VMEM)
        dma = pltpu.SemaphoreType.DMA
        act = (chunks, coefs, channels, LANES)
        wide = pltpu.VMEM((LANES * STEP, LANES), F32)
        pair = pltpu.VMEM((WIDE, pts, 2 * LANES), BF16)
        out_t, dx_t, d_up, d_gate, d_down = pl.pallas_call(
            fused_kernel,
            out_shape=(
                jax.ShapeDtypeStruct(x_t.shape, BF16),
                jax.ShapeDtypeStruct(x_t.shape, BF16),
                jax.ShapeDtypeStruct((degrees, hid, channels), BF16),
                jax.ShapeDtypeStruct((hid, channels), BF16),
                jax.ShapeDtypeStruct((degrees, hid, channels), BF16)),
            in_specs=[hbm] * 6 + [vmem] * 2,
            out_specs=(hbm, hbm, vmem, vmem, vmem),
            scratch_shapes=[
                pltpu.VMEM(act, BF16), pltpu.VMEM(act, BF16), pltpu.VMEM(act, BF16),
                pltpu.VMEM(act[1:], BF16), pltpu.VMEM(act[1:], BF16),
                wide, wide, wide, wide,
                pltpu.VMEM((degrees, hidden, channels), BF16), pltpu.VMEM((hidden, channels), BF16),
                pltpu.VMEM((degrees, hidden, channels), BF16), pltpu.VMEM((tp_size, degrees, share), F32),
                pltpu.VMEM((degrees, channels, hidden), BF16), pltpu.VMEM((channels, hidden), BF16),
                pltpu.VMEM((degrees, channels, hidden), BF16), pltpu.VMEM((degrees, channels, LANES), F32),
                pltpu.VMEM((pts, STEP), BF16), pltpu.VMEM((STEP, pts), BF16), pltpu.VMEM((pts, STEP), BF16), pltpu.VMEM((STEP, pts), BF16),
                pltpu.VMEM((LANES, 2 * LANES), F32), pair, pair, pair, pair,
                pltpu.VMEM((2 * degrees + 1, hidden, channels), F32), pltpu.VMEM((tp_size, 2 * degrees + 1, hid // 2, channels), F32),
                pltpu.VMEM((2, 2 * degrees + 1, hid // 2, channels), F32), pltpu.VMEM((2 * degrees + 1, hid // 2, channels), F32),
                pltpu.VMEM((2 * degrees + 1, hid, channels), BF16),
                dma((4, 4)), dma((4, 4)), dma((4,)),
                dma((2, chunks, 4)), dma((2, chunks, 4)), dma((2, chunks)),
                dma((2, chunks, 4)), dma((2, chunks, 4)), dma((2, chunks)),
                dma((tp_size + 4,)), dma((tp_size + 4,))],
            compiler_params=pltpu.CompilerParams(collective_id=0, has_side_effects=True, vmem_limit_bytes=62 * 1024 * 1024),
            name='fused',
        )(x_t, g_t, up_t, gate_t, down_loc, gain_loc, to_grid, jnp.transpose(from_grid, (1, 0)))
        back = lambda val: jnp.transpose(val, (2, 0, 1))

        return back(out_t), back(dx_t), jnp.transpose(d_up, (0, 2, 1)), jnp.transpose(d_gate, (1, 0)), d_down

    return jax.shard_map(local_step, mesh=mesh, in_specs=in_specs, out_specs=out_specs, check_vma=False)
```

```python
import jax
import jax.numpy as jnp
from jax import lax
from jax.experimental import pallas as pl
from jax.experimental.pallas import tpu as pltpu
from jax.sharding import PartitionSpec as P

NORM_EPS = 1e-5
F32 = jnp.float32
BF16 = jnp.bfloat16
MESH = pl.DeviceIdType.MESH
LANES = 128
STEP = 56
WIDE = 4


def degree_of(coef):
    total = (coef >= 1).astype(jnp.int32)
    for deg in range(2, 7):
        total = total + (coef >= deg * deg).astype(jnp.int32)
    return total


def mm(lhs, rhs):
    return jnp.dot(lhs, rhs, preferred_element_type=F32)


def mm_nt(lhs, rhs):
    return lax.dot_general(lhs, rhs, (((1,), (1,)), ((), ())), preferred_element_type=F32)


def sigmoid(val):
    return 0.5 * jnp.tanh(0.5 * val) + 0.5


def fused_kernel(x_hbm, g_hbm, up_hbm, gate_hbm, down_hbm, gain_hbm, tg_hbm, fg_hbm,
                 out_vm, dx_vm, fin_vm,
                 x_buf, g_buf, o_buf, n_buf, dn_buf, y0, y1, z0, z1,
                 wu, wg, wd, gain_in, wut, wgt, wdt, gain_b,
                 tt_ref, t_ref, f_ref, ft_ref, pad_buf, u_buf, s_buf, act_buf, du_buf,
                 g_sum, half_buf, mate_buf, far_buf, fin_buf,
                 tg_ref, fg_ref, w_send, w_recv, w_loc, in_send, in_recv, in_loc, o_send, o_recv, r_send, r_recv):
    chunks, coefs = x_buf.shape[0], x_buf.shape[1]
    share = x_hbm.shape[1]
    own = chunks * LANES
    me = lax.axis_index('tp')
    mate = me ^ 1
    side = lax.axis_index('dp')

    def rows(who, size):
        return pl.ds(pl.multiple_of(who * size, size), size)

    def lanes(who, chunk):
        return pl.ds(pl.multiple_of(who * own + chunk * LANES, LANES), LANES)

    barrier = pltpu.get_barrier_semaphore()
    for flip in (1, 2, 3):
        pl.semaphore_signal(barrier, inc=1, device_id={'tp': me ^ flip}, device_id_type=MESH)
    pl.semaphore_signal(barrier, inc=1, device_id={'dp': 1 - side}, device_id_type=MESH)
    pl.semaphore_signal(barrier, inc=1, device_id={'dp': 1 - side, 'tp': mate}, device_id_type=MESH)
    pl.semaphore_wait(barrier, 5)

    def weight_parts(who):
        hid = up_hbm.shape[1]
        return (wu.at[:, rows(who, hid), :], wd.at[:, rows(who, hid), :], wg.at[rows(who, hid), :], gain_in.at[who])

    sources = (up_hbm, down_hbm, gate_hbm, gain_hbm)

    def weight_copies(srcs, dsts, num, to, peer):
        return [pltpu.make_async_remote_copy(src, dst, w_send.at[to, i], w_recv.at[num, i], device_id=peer, device_id_type=MESH)
                for i, (src, dst) in enumerate(zip(srcs, dsts))]

    crosses = lax.rem(me, 2) == side
    mine, far = weight_parts(me), weight_parts(me ^ 2)
    own_weights = [pltpu.make_async_copy(src, dst, w_loc.at[i]) for i, (src, dst) in enumerate(zip(sources, mine))]
    far_weights = weight_copies(sources, mine, 2, 0, {'tp': me ^ 2})
    mate_weights = weight_copies(sources, mine, 1, 1, {'tp': mate})
    passed_weights = (weight_copies(far, far, 3, 2, {'tp': mate}) + weight_copies(far, far, 2, 3, {'dp': 1 - side})
                      + weight_copies(far, far, 3, 4, {'dp': 1 - side, 'tp': mate}))
    grids = [pltpu.make_async_copy(tg_hbm, tg_ref, w_loc.at[4]), pltpu.make_async_copy(fg_hbm, fg_ref, w_loc.at[5])]

    @pl.when(crosses)
    def _():
        for copy in far_weights:
            copy.start()

    for copy in mate_weights + own_weights + grids:
        copy.start()

    def input_copy(tensor, chunk, flip):
        src, buf = ((x_hbm, x_buf), (g_hbm, g_buf))[tensor]
        return pltpu.make_async_remote_copy(
            src.at[:, :, lanes(me ^ flip, chunk)], buf.at[chunk, :, rows(me, share), :],
            in_send.at[tensor, chunk, flip], in_recv.at[tensor, chunk, flip],
            device_id={'tp': me ^ flip}, device_id_type=MESH)

    def input_local(tensor, chunk):
        src, buf = ((x_hbm, x_buf), (g_hbm, g_buf))[tensor]
        return pltpu.make_async_copy(src.at[:, :, lanes(me, chunk)], buf.at[chunk, :, rows(me, share), :], in_loc.at[tensor, chunk])

    def output_copy(tensor, chunk, flip):
        buf, dst = ((o_buf, out_vm), (g_buf, dx_vm))[tensor]
        return pltpu.make_async_remote_copy(
            buf.at[chunk, :, rows(me ^ flip, share), :], dst.at[:, :, lanes(me, chunk)],
            o_send.at[tensor, chunk, flip], o_recv.at[tensor, chunk, flip],
            device_id={'tp': me ^ flip}, device_id_type=MESH)

    def output_local(tensor, chunk):
        buf, dst = ((o_buf, out_vm), (g_buf, dx_vm))[tensor]
        dst[:, :, lanes(me, chunk)] = buf[chunk, :, rows(me, share), :]

    def start_outputs(tensor, chunk):
        @pl.when(chunk < chunks - 1)
        def _():
            for flip in (2, 3):
                output_copy(tensor, chunk, flip).start()

        output_copy(tensor, chunk, 1).start()
        output_local(tensor, chunk)

    def start_inputs(chunk, carry):
        for flip in (2, 3, 1):
            for tensor in (0, 1):
                input_copy(tensor, chunk, flip).start()
        for tensor in (0, 1):
            input_local(tensor, chunk).start()
        return carry

    lax.fori_loop(0, chunks, start_inputs, 0)

    g_sum[...] = jnp.zeros_like(g_sum)
    blank = jnp.zeros((LANES, LANES), F32)
    for pad in range(coefs, STEP):
        for ref in (y0, y1, z0, z1):
            ref[pl.ds(pad, LANES, stride=STEP), :] = blank
    for ref in (z0, z1):
        ref[pl.ds(0, LANES, stride=STEP), :] = blank

    for copy in grids:
        copy.wait()
    points = tg_ref.shape[1]
    pts = t_ref.shape[1]
    pad_buf[...] = jnp.zeros_like(pad_buf)
    pad_buf[:coefs, :points] = tg_ref[...].astype(BF16).astype(F32)
    t_ref[...] = pad_buf[:STEP, :pts].astype(BF16)
    tt_ref[...] = (0.5 * pad_buf[...]).T[:pts, :STEP].astype(BF16)
    pad_buf[...] = jnp.zeros_like(pad_buf)
    pad_buf[1:coefs, :points] = fg_ref[...].astype(BF16).astype(F32)
    ft_ref[...] = pad_buf[:STEP, :pts].astype(BF16)
    f_ref[...] = (0.5 * pad_buf[...]).T[:pts, :STEP].astype(BF16)

    for copy in far_weights:
        copy.wait_recv()

    @pl.when(crosses)
    def _():
        for copy in passed_weights:
            copy.start()
        for copy in far_weights + passed_weights:
            copy.wait_send()

    for copy in passed_weights[:len(sources)]:
        copy.wait_recv()
    for copy in mate_weights + own_weights:
        copy.wait()

    def turn(deg, carry):
        wut[deg] = wu[deg].astype(F32).T.astype(BF16)
        wdt[deg] = wd[deg].astype(F32).T.astype(BF16)
        return carry

    degrees = wu.shape[0]
    lax.fori_loop(0, degrees, turn, 0)
    wgt[...] = wg[...].astype(F32).T.astype(BF16)
    gains = jnp.concatenate([gain_in[i] for i in range(gain_in.shape[0])], axis=1)
    pad_buf[:degrees, :LANES] = gains
    gains = pad_buf[:, :LANES].T
    for deg in range(degrees):
        gain_b[deg] = jnp.broadcast_to(gains[:, deg:deg + 1], (LANES, LANES))

    inv_chan = 1.0 / LANES
    inv_vec = 1.0 / (LANES * (coefs - 1))

    def chunk_step(chunk, carry):
        for flip in (2, 3, 1):
            for tensor in (0, 1):
                input_copy(tensor, chunk, flip).wait_recv()
        for tensor in (0, 1):
            input_local(tensor, chunk).wait()

        def square_sum(k, acc):
            val = x_buf[chunk, k].astype(F32)
            return acc + val * val

        sq = lax.fori_loop(1, coefs, square_sum, jnp.zeros((LANES, LANES), F32), unroll=8)
        inv_v = lax.rsqrt(jnp.sum(sq, axis=0, keepdims=True) * inv_vec + NORM_EPS)
        scalar = x_buf[chunk, 0].astype(F32)
        cent = scalar - jnp.sum(scalar, axis=0, keepdims=True) * inv_chan
        inv_s = lax.rsqrt(jnp.sum(cent * cent, axis=0, keepdims=True) * inv_chan + NORM_EPS)
        hat_s = cent * inv_s
        n_zero = (hat_s * gain_b[0]).astype(BF16)
        n_buf[0] = n_zero
        y_zero = mm(wu[0], n_zero)
        y0[pl.ds(0, LANES, stride=STEP), :] = y_zero[:LANES]
        y1[pl.ds(0, LANES, stride=STEP), :] = y_zero[LANES:]

        def up_step(k, carry):
            deg = degree_of(k)
            n_k = (x_buf[chunk, k].astype(F32) * inv_v * gain_b[deg]).astype(BF16)
            n_buf[k] = n_k
            y_k = mm(wu[deg], n_k)
            y0[pl.ds(k, LANES, stride=STEP), :] = y_k[:LANES]
            y1[pl.ds(k, LANES, stride=STEP), :] = y_k[LANES:]
            dm_k = mm(wd[deg], g_buf[chunk, k])
            z0[pl.ds(k, LANES, stride=STEP), :] = dm_k[:LANES]
            z1[pl.ds(k, LANES, stride=STEP), :] = dm_k[LANES:]
            return carry

        lax.fori_loop(1, coefs, up_step, 0, unroll=4)

        groups = LANES // WIDE

        def spans_of(group):
            return [pl.ds(pl.multiple_of((group * WIDE + i) * STEP, 8), STEP) for i in range(WIDE)]

        def grid_step(i, carry):
            late = spans_of(jnp.maximum(i - 2, 0))
            early = spans_of(jnp.minimum(i, groups - 1))
            ys = [jnp.concatenate([y0[span, :], y1[span, :]], axis=1).astype(BF16) for span in early]
            dms = [jnp.concatenate([z0[span, :], z1[span, :]], axis=1).astype(BF16) for span in early]
            zs = [mm(ft_ref[...], act_buf[n]) for n in range(WIDE)]
            dys = [mm(t_ref[...], du_buf[n]) for n in range(WIDE)]
            for n in range(WIDE):
                half = u_buf[n].astype(F32)
                tan = jnp.tanh(half)
                both = half * tan
                act_buf[n] = (half + both).astype(BF16)
                du_buf[n] = (s_buf[n].astype(F32) * ((1.0 + tan) + (half - both * tan))).astype(BF16)
            for n in range(WIDE):
                u_buf[n] = mm(tt_ref[...], ys[n]).astype(BF16)
                s_buf[n] = mm(f_ref[...], dms[n]).astype(BF16)
            for span, z_j, dy_j in zip(late, zs, dys):
                z0[span, :] = z_j[:, :LANES]
                z1[span, :] = z_j[:, LANES:]
                y0[span, :] = dy_j[:, :LANES]
                y1[span, :] = dy_j[:, LANES:]
            return carry

        lax.fori_loop(0, groups + 2, grid_step, 0)

        def hidden_grad(k):
            picked = pl.ds(k, LANES, stride=STEP)
            return jnp.concatenate([y0[picked, :], y1[picked, :]], axis=0).astype(BF16)

        g_zero = g_buf[chunk, 0]
        n_zero = n_buf[0]
        pre = mm(wg[...], n_zero).astype(BF16).astype(F32)
        sig = sigmoid(pre)
        gate = pre * sig
        dm_zero = mm(wd[0], g_zero).astype(BF16).astype(F32)
        d_pre = (dm_zero * (sig + gate * (1.0 - sig))).astype(BF16)
        gate = gate.astype(BF16)
        o_buf[chunk, 0] = (x_buf[chunk, 0].astype(F32) + mm(wdt[0], gate)).astype(BF16)
        g_sum[degrees] += mm_nt(gate, g_zero)
        dy_zero = hidden_grad(0)
        g_sum[0] += mm_nt(dy_zero, n_zero)
        g_sum[2 * degrees] += mm_nt(d_pre, n_zero)
        dn_zero = (mm(wut[0], dy_zero) + mm(wgt[...], d_pre)).astype(BF16).astype(F32)

        def down_step(k, acc):
            deg = degree_of(k)
            picked = pl.ds(k, LANES, stride=STEP)
            m_k = jnp.concatenate([z0[picked, :], z1[picked, :]], axis=0).astype(BF16)
            dy_k = hidden_grad(k)
            x_k = x_buf[chunk, k].astype(F32)
            o_buf[chunk, k] = (x_k + mm(wdt[deg], m_k)).astype(BF16)
            g_sum[degrees + deg] += mm_nt(m_k, g_buf[chunk, k])
            dn_k = mm(wut[deg], dy_k).astype(BF16)
            dn_buf[k] = dn_k
            g_sum[deg] += mm_nt(dy_k, n_buf[k])
            return acc + dn_k.astype(F32) * gain_b[deg] * x_k

        dot_v = lax.fori_loop(1, coefs, down_step, jnp.zeros((LANES, LANES), F32), unroll=4)
        start_outputs(0, chunk)

        z0[pl.ds(0, LANES, stride=STEP), :] = blank
        z1[pl.ds(0, LANES, stride=STEP), :] = blank
        dh_s = dn_zero * gain_b[0]
        mean_d = jnp.sum(dh_s, axis=0, keepdims=True) * inv_chan
        mean_dx = jnp.sum(dh_s * hat_s, axis=0, keepdims=True) * inv_chan
        dx_s = inv_s * (dh_s - mean_d - hat_s * mean_dx)
        g_buf[chunk, 0] = (dx_s + g_zero.astype(F32)).astype(BF16)
        coef_v = inv_v * inv_v * inv_v * (jnp.sum(dot_v, axis=0, keepdims=True) * inv_vec)

        def back_step(k, carry):
            dh = dn_buf[k].astype(F32) * gain_b[degree_of(k)]
            dx = inv_v * dh - x_buf[chunk, k].astype(F32) * coef_v
            g_buf[chunk, k] = (dx + g_buf[chunk, k].astype(F32)).astype(BF16)
            return carry

        lax.fori_loop(1, coefs, back_step, 0, unroll=4)
        start_outputs(1, chunk)
        return carry

    lax.fori_loop(0, chunks, chunk_step, 0)

    hid = up_hbm.shape[1]
    part = hid // 2
    slices = half_buf.shape[0]

    def sum_rows(who, where):
        return pl.ds(pl.multiple_of(who * hid + where * part, part), part)

    def push(src, dst, num, peer):
        return pltpu.make_async_remote_copy(src, dst, r_send.at[num], r_recv.at[num], device_id=peer, device_id_type=MESH)

    halves = [push(g_sum.at[:, sum_rows(n, 1 - side), :], half_buf.at[n], n, {'dp': 1 - side}) for n in range(slices)]
    for copy in halves:
        copy.start()
    for copy in halves:
        copy.wait_recv()
    rows_all = g_sum.shape[0]

    def add_half(row, carry):
        for n in range(slices):
            half_buf[n, row] += g_sum[row, sum_rows(n, side), :]
        return carry

    lax.fori_loop(0, rows_all, add_half, 0)
    shares = [push(half_buf.at[mate], mate_buf.at[0], slices, {'tp': mate}),
              push(half_buf.at[mate ^ 2], mate_buf.at[1], slices + 1, {'tp': mate})]
    for copy in shares:
        copy.start()
    for copy in shares:
        copy.wait()

    def add_mate(row, carry):
        mate_buf[0, row] += half_buf[me, row]
        mate_buf[1, row] += half_buf[me ^ 2, row]
        return carry

    lax.fori_loop(0, rows_all, add_mate, 0)
    cross = push(mate_buf.at[1], far_buf, slices + 2, {'tp': me ^ 2})
    cross.start()
    for tensor in (0, 1):
        for flip in (2, 3):
            output_copy(tensor, chunks - 1, flip).start()
    cross.wait()
    ours = pl.ds(pl.multiple_of(side * part, part), part)

    def add_far(row, carry):
        fin_buf[row, ours, :] = (mate_buf[0, row] + far_buf[row]).astype(BF16)
        return carry

    lax.fori_loop(0, rows_all, add_far, 0)
    last = push(fin_buf.at[:, ours, :], fin_buf.at[:, ours, :], slices + 3, {'dp': 1 - side})
    last.start()
    last.wait()
    for copy in halves:
        copy.wait_send()
    fin_vm[...] = fin_buf[...]

    def finish(chunk, carry):
        for tensor in (0, 1):
            for flip in (2, 3, 1):
                input_copy(tensor, chunk, flip).wait_send()
                output_copy(tensor, chunk, flip).wait()
        return carry

    lax.fori_loop(0, chunks, finish, 0)


def write_kernel(out_vm, dx_vm, fin_vm, out_hbm, dx_hbm, dup_hbm, dgate_hbm, ddown_hbm, sems, small):
    coefs, step = out_hbm.shape[0], 7
    degrees = dup_hbm.shape[0]
    copies = []
    for start in range(0, coefs, step):
        span = pl.ds(start, step)
        copies.append(pltpu.make_async_copy(out_vm.at[span], out_hbm.at[span], sems.at[0, start]))
        copies.append(pltpu.make_async_copy(dx_vm.at[span], dx_hbm.at[span], sems.at[1, start]))
    copies.append(pltpu.make_async_copy(fin_vm.at[pl.ds(0, degrees)], dup_hbm, small.at[0]))
    copies.append(pltpu.make_async_copy(fin_vm.at[pl.ds(degrees, degrees)], ddown_hbm, small.at[1]))
    copies.append(pltpu.make_async_copy(fin_vm.at[2 * degrees], dgate_hbm, small.at[2]))
    for copy in copies:
        copy.start()
    for copy in copies:
        copy.wait()


def solution(mesh):
    tp_size = mesh.shape['tp']
    act_spec = P('dp', None, 'tp')
    in_specs = (act_spec, P(None, 'tp'), P(None, None, 'tp'), P(None, 'tp'), P(None, 'tp', None), P(None, None), P(None, None), act_spec)
    out_specs = (act_spec, act_spec, P(None, None, 'tp'), P(None, 'tp'), P(None, 'tp', None))

    def local_step(x_loc, gain_loc, up_loc, gate_loc, down_loc, to_grid, from_grid, grad_loc):
        nodes, coefs, share = x_loc.shape
        degrees, channels, hid = up_loc.shape
        hidden = hid * tp_size
        points = to_grid.shape[1]
        pts = -(-points // 8) * 8
        chunks = nodes // tp_size // LANES
        x_t = jnp.transpose(x_loc, (1, 2, 0))
        g_t = jnp.transpose(grad_loc, (1, 2, 0))
        up_t = jnp.transpose(up_loc, (0, 2, 1))
        gate_t = jnp.transpose(gate_loc, (1, 0))
        hbm = pl.BlockSpec(memory_space=pl.ANY)
        vmem = pl.BlockSpec(memory_space=pltpu.VMEM)
        dma = pltpu.SemaphoreType.DMA
        act = (chunks, coefs, channels, LANES)
        wide = pltpu.VMEM((LANES * STEP, LANES), F32)
        pair = pltpu.VMEM((WIDE, pts, 2 * LANES), BF16)
        out_v, dx_v, fin_v = pl.pallas_call(
            fused_kernel,
            out_shape=(pltpu.VMEM(x_t.shape, BF16), pltpu.VMEM(x_t.shape, BF16), pltpu.VMEM((2 * degrees + 1, hid, channels), BF16)),
            in_specs=[hbm] * 8,
            out_specs=(vmem, vmem, vmem),
            scratch_shapes=[
                pltpu.VMEM(act, BF16), pltpu.VMEM(act, BF16), pltpu.VMEM(act, BF16),
                pltpu.VMEM(act[1:], BF16), pltpu.VMEM(act[1:], BF16),
                wide, wide, wide, wide,
                pltpu.VMEM((degrees, hidden, channels), BF16), pltpu.VMEM((hidden, channels), BF16),
                pltpu.VMEM((degrees, hidden, channels), BF16), pltpu.VMEM((tp_size, degrees, share), F32),
                pltpu.VMEM((degrees, channels, hidden), BF16), pltpu.VMEM((channels, hidden), BF16),
                pltpu.VMEM((degrees, channels, hidden), BF16), pltpu.VMEM((degrees, channels, LANES), F32),
                pltpu.VMEM((pts, STEP), BF16), pltpu.VMEM((STEP, pts), BF16), pltpu.VMEM((pts, STEP), BF16), pltpu.VMEM((STEP, pts), BF16),
                pltpu.VMEM((LANES, 2 * LANES), F32), pair, pair, pair, pair,
                pltpu.VMEM((2 * degrees + 1, hidden, channels), F32), pltpu.VMEM((tp_size, 2 * degrees + 1, hid // 2, channels), F32),
                pltpu.VMEM((2, 2 * degrees + 1, hid // 2, channels), F32), pltpu.VMEM((2 * degrees + 1, hid // 2, channels), F32),
                pltpu.VMEM((2 * degrees + 1, hid, channels), BF16),
                pltpu.VMEM(to_grid.shape, F32), pltpu.VMEM(from_grid.shape[::-1], F32),
                dma((5, 4)), dma((4, 4)), dma((6,)),
                dma((2, chunks, 4)), dma((2, chunks, 4)), dma((2, chunks)),
                dma((2, chunks, 4)), dma((2, chunks, 4)),
                dma((tp_size + 4,)), dma((tp_size + 4,))],
            compiler_params=pltpu.CompilerParams(collective_id=0, has_side_effects=True, vmem_limit_bytes=48 * 1024 * 1024),
            name='fused',
        )(x_t, g_t, up_t, gate_t, down_loc, gain_loc, to_grid, jnp.transpose(from_grid, (1, 0)))
        out_t, dx_t, d_up, d_gate, d_down = pl.pallas_call(
            write_kernel,
            out_shape=(
                jax.ShapeDtypeStruct(x_t.shape, BF16),
                jax.ShapeDtypeStruct(x_t.shape, BF16),
                jax.ShapeDtypeStruct((degrees, hid, channels), BF16),
                jax.ShapeDtypeStruct((hid, channels), BF16),
                jax.ShapeDtypeStruct((degrees, hid, channels), BF16)),
            in_specs=[vmem] * 3,
            out_specs=(hbm,) * 5,
            scratch_shapes=[dma((2, coefs)), dma((3,))],
            compiler_params=pltpu.CompilerParams(vmem_limit_bytes=1024 * 1024),
            name='write',
        )(out_v, dx_v, fin_v)
        back = lambda val: jnp.transpose(val, (2, 0, 1))
        return back(out_t), back(dx_t), jnp.transpose(d_up, (0, 2, 1)), jnp.transpose(d_gate, (1, 0)), d_down

    return jax.shard_map(local_step, mesh=mesh, in_specs=in_specs, out_specs=out_specs, check_vma=False)
```

```python
import jax
import jax.numpy as jnp
from jax import lax
from jax.experimental import pallas as pl
from jax.experimental.pallas import tpu as pltpu
from jax.sharding import PartitionSpec as P

NORM_EPS = 1e-5
F32 = jnp.float32
BF16 = jnp.bfloat16
MESH = pl.DeviceIdType.MESH
LANES = 128
STEP = 56
WIDE = 4


def degree_of(coef):
    total = (coef >= 1).astype(jnp.int32)
    for deg in range(2, 7):
        total = total + (coef >= deg * deg).astype(jnp.int32)
    return total


def mm(lhs, rhs):
    return jnp.dot(lhs, rhs, preferred_element_type=F32)


def mm_nt(lhs, rhs):
    return lax.dot_general(lhs, rhs, (((1,), (1,)), ((), ())), preferred_element_type=F32)


def sigmoid(val):
    return 0.5 * jnp.tanh(0.5 * val) + 0.5


def fused_kernel(x_hbm, g_hbm, up_hbm, gate_hbm, down_hbm, gain_hbm, tg_hbm, fg_hbm,
                 out_vm, dx_vm, fin_vm,
                 x_buf, g_buf, o_buf, n_buf, dn_buf, y0, y1, z0, z1,
                 wu, wg, wd, gain_in, wut, wgt, wdt, gain_b,
                 tt_ref, t_ref, f_ref, ft_ref, pad_buf, u_buf, s_buf, act_buf, du_buf,
                 g_sum, half_buf, mate_buf, far_buf, fin_buf,
                 tg_ref, fg_ref, w_send, w_recv, w_loc, in_send, in_recv, o_send, o_recv, r_send, r_recv):
    chunks, coefs = x_buf.shape[0], x_buf.shape[1]
    share = x_hbm.shape[1]
    own = chunks * LANES
    me = lax.axis_index('tp')
    mate = me ^ 1
    side = lax.axis_index('dp')

    def rows(who, size):
        return pl.ds(pl.multiple_of(who * size, size), size)

    def lanes(who, chunk):
        return pl.ds(pl.multiple_of(who * own + chunk * LANES, LANES), LANES)

    def drain(ref, sem):
        pltpu.make_async_copy(ref, ref, sem).wait()

    barrier = pltpu.get_barrier_semaphore()
    for flip in (1, 2, 3):
        pl.semaphore_signal(barrier, inc=1, device_id={'tp': me ^ flip}, device_id_type=MESH)
    pl.semaphore_signal(barrier, inc=1, device_id={'dp': 1 - side}, device_id_type=MESH)
    pl.semaphore_signal(barrier, inc=1, device_id={'dp': 1 - side, 'tp': mate}, device_id_type=MESH)
    pl.semaphore_wait(barrier, 5)

    def weight_parts(who):
        hid = up_hbm.shape[1]
        return (wu.at[:, rows(who, hid), :], wd.at[:, rows(who, hid), :], wg.at[rows(who, hid), :], gain_in.at[who])

    sources = (up_hbm, down_hbm, gate_hbm, gain_hbm)

    def weight_copies(srcs, dsts, come, to, peer):
        return [pltpu.make_async_remote_copy(src, dst, w_send.at[to, i], w_recv.at[come, i], device_id=peer, device_id_type=MESH)
                for i, (src, dst) in enumerate(zip(srcs, dsts))]

    crosses = lax.rem(me, 2) == side
    mine, far = weight_parts(me), weight_parts(me ^ 2)
    own_weights = [pltpu.make_async_copy(src, dst, w_loc.at[0, i]) for i, (src, dst) in enumerate(zip(sources, mine))]
    far_weights = weight_copies(sources, mine, 0, 0, {'tp': me ^ 2})
    mate_weights = weight_copies(sources, mine, 1, 1, {'tp': mate})
    passed_weights = (weight_copies(far, far, 2, 2, {'tp': mate}) + weight_copies(far, far, 0, 2, {'dp': 1 - side})
                      + weight_copies(far, far, 2, 2, {'dp': 1 - side, 'tp': mate}))
    hid = up_hbm.shape[1]
    thrice = (wu.at[:, pl.ds(0, 3 * hid), :], wd.at[:, pl.ds(0, 3 * hid), :], wg.at[pl.ds(0, 3 * hid), :], gain_in.at[pl.ds(0, 3)])
    grids = [pltpu.make_async_copy(tg_hbm, tg_ref, w_loc.at[1, 0]), pltpu.make_async_copy(fg_hbm, fg_ref, w_loc.at[1, 1])]

    @pl.when(crosses)
    def _():
        for copy in far_weights:
            copy.start()

    for copy in mate_weights + own_weights + grids:
        copy.start()

    def input_copy(tensor, chunk, flip):
        src, buf = ((x_hbm, x_buf), (g_hbm, g_buf))[tensor]
        return pltpu.make_async_remote_copy(
            src.at[:, :, lanes(me ^ flip, chunk)], buf.at[chunk, :, rows(me, share), :],
            in_send.at[tensor], in_recv.at[tensor, chunk],
            device_id={'tp': me ^ flip}, device_id_type=MESH)

    def input_local(tensor, chunk):
        src, buf = ((x_hbm, x_buf), (g_hbm, g_buf))[tensor]
        return pltpu.make_async_copy(src.at[:, :, lanes(me, chunk)], buf.at[chunk, :, rows(me, share), :], in_recv.at[tensor, chunk])

    def output_copy(tensor, chunk, flip):
        buf, dst = ((o_buf, out_vm), (g_buf, dx_vm))[tensor]
        return pltpu.make_async_remote_copy(
            buf.at[chunk, :, rows(me ^ flip, share), :], dst.at[:, :, lanes(me, chunk)],
            o_send.at[tensor], o_recv.at[tensor],
            device_id={'tp': me ^ flip}, device_id_type=MESH)

    def output_local(tensor, chunk):
        buf, dst = ((o_buf, out_vm), (g_buf, dx_vm))[tensor]
        dst[:, :, lanes(me, chunk)] = buf[chunk, :, rows(me, share), :]

    def start_outputs(tensor, chunk):
        @pl.when(chunk < chunks - 1)
        def _():
            for flip in (2, 3):
                output_copy(tensor, chunk, flip).start()

        output_copy(tensor, chunk, 1).start()
        output_local(tensor, chunk)

    def start_inputs(chunk, carry):
        for flip in (2, 3, 1):
            for tensor in (0, 1):
                input_copy(tensor, chunk, flip).start()
        for tensor in (0, 1):
            input_local(tensor, chunk).start()
        return carry

    lax.fori_loop(0, chunks, start_inputs, 0)

    g_sum[...] = jnp.zeros_like(g_sum)
    blank = jnp.zeros((LANES, LANES), F32)
    for pad in range(coefs, STEP):
        for ref in (y0, y1, z0, z1):
            ref[pl.ds(pad, LANES, stride=STEP), :] = blank
    for ref in (z0, z1):
        ref[pl.ds(0, LANES, stride=STEP), :] = blank

    for copy in grids:
        copy.wait()
    points = tg_ref.shape[1]
    pts = t_ref.shape[1]
    pad_buf[...] = jnp.zeros_like(pad_buf)
    pad_buf[:coefs, :points] = tg_ref[...].astype(BF16).astype(F32)
    t_ref[...] = pad_buf[:STEP, :pts].astype(BF16)
    tt_ref[...] = (0.5 * pad_buf[...]).T[:pts, :STEP].astype(BF16)
    pad_buf[...] = jnp.zeros_like(pad_buf)
    pad_buf[1:coefs, :points] = fg_ref[...].astype(BF16).astype(F32)
    ft_ref[...] = pad_buf[:STEP, :pts].astype(BF16)
    f_ref[...] = (0.5 * pad_buf[...]).T[:pts, :STEP].astype(BF16)

    for copy in far_weights:
        copy.wait_recv()

    @pl.when(crosses)
    def _():
        for copy in passed_weights:
            copy.start()
        for i, copy in enumerate(far_weights):
            copy.wait_send()
            drain(thrice[i], w_send.at[2, i])

    for copy in passed_weights[:len(sources)]:
        copy.wait_recv()
    for copy in mate_weights + own_weights:
        copy.wait()

    def turn(deg, carry):
        wut[deg] = wu[deg].astype(F32).T.astype(BF16)
        wdt[deg] = wd[deg].astype(F32).T.astype(BF16)
        return carry

    degrees = wu.shape[0]
    lax.fori_loop(0, degrees, turn, 0)
    wgt[...] = wg[...].astype(F32).T.astype(BF16)
    gains = jnp.concatenate([gain_in[i] for i in range(gain_in.shape[0])], axis=1)
    pad_buf[:degrees, :LANES] = gains
    gains = pad_buf[:, :LANES].T
    for deg in range(degrees):
        gain_b[deg] = jnp.broadcast_to(gains[:, deg:deg + 1], (LANES, LANES))

    inv_chan = 1.0 / LANES
    inv_vec = 1.0 / (LANES * (coefs - 1))

    def chunk_step(chunk, carry):
        for tensor, buf in enumerate((x_buf, g_buf)):
            drain(buf.at[chunk], in_recv.at[tensor, chunk])

        def square_sum(k, acc):
            val = x_buf[chunk, k].astype(F32)
            return acc + val * val

        sq = lax.fori_loop(1, coefs, square_sum, jnp.zeros((LANES, LANES), F32), unroll=8)
        inv_v = lax.rsqrt(jnp.sum(sq, axis=0, keepdims=True) * inv_vec + NORM_EPS)
        scalar = x_buf[chunk, 0].astype(F32)
        cent = scalar - jnp.sum(scalar, axis=0, keepdims=True) * inv_chan
        inv_s = lax.rsqrt(jnp.sum(cent * cent, axis=0, keepdims=True) * inv_chan + NORM_EPS)
        hat_s = cent * inv_s
        n_zero = (hat_s * gain_b[0]).astype(BF16)
        n_buf[0] = n_zero
        y_zero = mm(wu[0], n_zero)
        y0[pl.ds(0, LANES, stride=STEP), :] = y_zero[:LANES]
        y1[pl.ds(0, LANES, stride=STEP), :] = y_zero[LANES:]

        def up_step(k, carry):
            deg = degree_of(k)
            n_k = (x_buf[chunk, k].astype(F32) * inv_v * gain_b[deg]).astype(BF16)
            n_buf[k] = n_k
            y_k = mm(wu[deg], n_k)
            y0[pl.ds(k, LANES, stride=STEP), :] = y_k[:LANES]
            y1[pl.ds(k, LANES, stride=STEP), :] = y_k[LANES:]
            dm_k = mm(wd[deg], g_buf[chunk, k])
            z0[pl.ds(k, LANES, stride=STEP), :] = dm_k[:LANES]
            z1[pl.ds(k, LANES, stride=STEP), :] = dm_k[LANES:]
            return carry

        lax.fori_loop(1, coefs, up_step, 0, unroll=4)

        groups = LANES // WIDE

        def spans_of(group):
            return [pl.ds(pl.multiple_of((group * WIDE + i) * STEP, 8), STEP) for i in range(WIDE)]

        def grid_step(i, carry):
            late = spans_of(jnp.maximum(i - 2, 0))
            early = spans_of(jnp.minimum(i, groups - 1))
            ys = [jnp.concatenate([y0[span, :], y1[span, :]], axis=1).astype(BF16) for span in early]
            dms = [jnp.concatenate([z0[span, :], z1[span, :]], axis=1).astype(BF16) for span in early]
            zs = [mm(ft_ref[...], act_buf[n]) for n in range(WIDE)]
            dys = [mm(t_ref[...], du_buf[n]) for n in range(WIDE)]
            for n in range(WIDE):
                half = u_buf[n].astype(F32)
                tan = jnp.tanh(half)
                both = half * tan
                act_buf[n] = (half + both).astype(BF16)
                du_buf[n] = (s_buf[n].astype(F32) * ((1.0 + tan) + (half - both * tan))).astype(BF16)
            for n in range(WIDE):
                u_buf[n] = mm(tt_ref[...], ys[n]).astype(BF16)
                s_buf[n] = mm(f_ref[...], dms[n]).astype(BF16)
            for span, z_j, dy_j in zip(late, zs, dys):
                z0[span, :] = z_j[:, :LANES]
                z1[span, :] = z_j[:, LANES:]
                y0[span, :] = dy_j[:, :LANES]
                y1[span, :] = dy_j[:, LANES:]
            return carry

        lax.fori_loop(0, groups + 2, grid_step, 0)

        def hidden_grad(k):
            picked = pl.ds(k, LANES, stride=STEP)
            return jnp.concatenate([y0[picked, :], y1[picked, :]], axis=0).astype(BF16)

        g_zero = g_buf[chunk, 0]
        n_zero = n_buf[0]
        pre = mm(wg[...], n_zero).astype(BF16).astype(F32)
        sig = sigmoid(pre)
        gate = pre * sig
        dm_zero = mm(wd[0], g_zero).astype(BF16).astype(F32)
        d_pre = (dm_zero * (sig + gate * (1.0 - sig))).astype(BF16)
        gate = gate.astype(BF16)
        o_buf[chunk, 0] = (x_buf[chunk, 0].astype(F32) + mm(wdt[0], gate)).astype(BF16)
        g_sum[degrees] += mm_nt(gate, g_zero)
        dy_zero = hidden_grad(0)
        g_sum[0] += mm_nt(dy_zero, n_zero)
        g_sum[2 * degrees] += mm_nt(d_pre, n_zero)
        dn_zero = (mm(wut[0], dy_zero) + mm(wgt[...], d_pre)).astype(BF16).astype(F32)

        def down_step(k, acc):
            deg = degree_of(k)
            picked = pl.ds(k, LANES, stride=STEP)
            m_k = jnp.concatenate([z0[picked, :], z1[picked, :]], axis=0).astype(BF16)
            dy_k = hidden_grad(k)
            x_k = x_buf[chunk, k].astype(F32)
            o_buf[chunk, k] = (x_k + mm(wdt[deg], m_k)).astype(BF16)
            g_sum[degrees + deg] += mm_nt(m_k, g_buf[chunk, k])
            dn_k = mm(wut[deg], dy_k).astype(BF16)
            dn_buf[k] = dn_k
            g_sum[deg] += mm_nt(dy_k, n_buf[k])
            return acc + dn_k.astype(F32) * gain_b[deg] * x_k

        dot_v = lax.fori_loop(1, coefs, down_step, jnp.zeros((LANES, LANES), F32), unroll=4)
        start_outputs(0, chunk)

        z0[pl.ds(0, LANES, stride=STEP), :] = blank
        z1[pl.ds(0, LANES, stride=STEP), :] = blank
        dh_s = dn_zero * gain_b[0]
        mean_d = jnp.sum(dh_s, axis=0, keepdims=True) * inv_chan
        mean_dx = jnp.sum(dh_s * hat_s, axis=0, keepdims=True) * inv_chan
        dx_s = inv_s * (dh_s - mean_d - hat_s * mean_dx)
        g_buf[chunk, 0] = (dx_s + g_zero.astype(F32)).astype(BF16)
        coef_v = inv_v * inv_v * inv_v * (jnp.sum(dot_v, axis=0, keepdims=True) * inv_vec)

        def back_step(k, carry):
            dh = dn_buf[k].astype(F32) * gain_b[degree_of(k)]
            dx = inv_v * dh - x_buf[chunk, k].astype(F32) * coef_v
            g_buf[chunk, k] = (dx + g_buf[chunk, k].astype(F32)).astype(BF16)
            return carry

        lax.fori_loop(1, coefs, back_step, 0, unroll=4)
        start_outputs(1, chunk)
        return carry

    lax.fori_loop(0, chunks, chunk_step, 0)

    part = hid // 2
    slices = half_buf.shape[0]

    def sum_rows(who, where):
        return pl.ds(pl.multiple_of(who * hid + where * part, part), part)

    def push(src, dst, num, peer):
        return pltpu.make_async_remote_copy(src, dst, r_send.at[num], r_recv.at[num], device_id=peer, device_id_type=MESH)

    for n in range(slices):
        push(g_sum.at[:, sum_rows(n, 1 - side), :], half_buf.at[n], 0, {'dp': 1 - side}).start()
    drain(half_buf, r_recv.at[0])
    rows_all = g_sum.shape[0]

    def add_half(row, carry):
        for n in range(slices):
            half_buf[n, row] += g_sum[row, sum_rows(n, side), :]
        return carry

    lax.fori_loop(0, rows_all, add_half, 0)
    push(half_buf.at[mate], mate_buf.at[0], 1, {'tp': mate}).start()
    push(half_buf.at[mate ^ 2], mate_buf.at[1], 1, {'tp': mate}).start()
    drain(mate_buf, r_recv.at[1])
    drain(mate_buf, r_send.at[1])

    def add_mate(row, carry):
        mate_buf[0, row] += half_buf[me, row]
        mate_buf[1, row] += half_buf[me ^ 2, row]
        return carry

    lax.fori_loop(0, rows_all, add_mate, 0)
    cross = push(mate_buf.at[1], far_buf, 2, {'tp': me ^ 2})
    cross.start()
    for tensor in (0, 1):
        for flip in (2, 3):
            output_copy(tensor, chunks - 1, flip).start()
    cross.wait()
    ours = pl.ds(pl.multiple_of(side * part, part), part)

    def add_far(row, carry):
        fin_buf[row, ours, :] = (mate_buf[0, row] + far_buf[row]).astype(BF16)
        return carry

    lax.fori_loop(0, rows_all, add_far, 0)
    last = push(fin_buf.at[:, ours, :], fin_buf.at[:, ours, :], 3, {'dp': 1 - side})
    last.start()
    last.wait()
    drain(half_buf, r_send.at[0])
    fin_vm[...] = fin_buf[...]

    for tensor, (buf, dst) in enumerate(((o_buf, out_vm), (g_buf, dx_vm))):
        sent = buf.at[:, :, pl.ds(0, LANES - share), :]
        drain(sent, in_send.at[tensor])
        drain(sent, o_send.at[tensor])
        drain(dst.at[:, :, pl.ds(0, x_hbm.shape[2] - own)], o_recv.at[tensor])


def write_kernel(out_vm, dx_vm, fin_vm, out_hbm, dx_hbm, dup_hbm, dgate_hbm, ddown_hbm, sems):
    coefs, step = out_hbm.shape[0], 7
    degrees = dup_hbm.shape[0]
    for start in range(0, coefs, step):
        span = pl.ds(start, step)
        pltpu.make_async_copy(out_vm.at[span], out_hbm.at[span], sems.at[0]).start()
        pltpu.make_async_copy(dx_vm.at[span], dx_hbm.at[span], sems.at[1]).start()
    small = [pltpu.make_async_copy(fin_vm.at[pl.ds(0, degrees)], dup_hbm, sems.at[2]),
             pltpu.make_async_copy(fin_vm.at[pl.ds(degrees, degrees)], ddown_hbm, sems.at[3]),
             pltpu.make_async_copy(fin_vm.at[2 * degrees], dgate_hbm, sems.at[4])]
    for copy in small:
        copy.start()
    for copy in small:
        copy.wait()
    pltpu.make_async_copy(out_vm, out_hbm, sems.at[0]).wait()
    pltpu.make_async_copy(dx_vm, dx_hbm, sems.at[1]).wait()


def solution(mesh):
    tp_size = mesh.shape['tp']
    act_spec = P('dp', None, 'tp')
    in_specs = (act_spec, P(None, 'tp'), P(None, None, 'tp'), P(None, 'tp'), P(None, 'tp', None), P(None, None), P(None, None), act_spec)
    out_specs = (act_spec, act_spec, P(None, None, 'tp'), P(None, 'tp'), P(None, 'tp', None))

    def local_step(x_loc, gain_loc, up_loc, gate_loc, down_loc, to_grid, from_grid, grad_loc):
        nodes, coefs, share = x_loc.shape
        degrees, channels, hid = up_loc.shape
        hidden = hid * tp_size
        points = to_grid.shape[1]
        pts = -(-points // 8) * 8
        chunks = nodes // tp_size // LANES
        x_t = jnp.transpose(x_loc, (1, 2, 0))
        g_t = jnp.transpose(grad_loc, (1, 2, 0))
        up_t = jnp.transpose(up_loc, (0, 2, 1))
        gate_t = jnp.transpose(gate_loc, (1, 0))
        hbm = pl.BlockSpec(memory_space=pl.ANY)
        vmem = pl.BlockSpec(memory_space=pltpu.VMEM)
        dma = pltpu.SemaphoreType.DMA
        act = (chunks, coefs, channels, LANES)
        wide = pltpu.VMEM((LANES * STEP, LANES), F32)
        pair = pltpu.VMEM((WIDE, pts, 2 * LANES), BF16)
        out_v, dx_v, fin_v = pl.pallas_call(
            fused_kernel,
            out_shape=(pltpu.VMEM(x_t.shape, BF16), pltpu.VMEM(x_t.shape, BF16), pltpu.VMEM((2 * degrees + 1, hid, channels), BF16)),
            in_specs=[hbm] * 8,
            out_specs=(vmem, vmem, vmem),
            scratch_shapes=[
                pltpu.VMEM(act, BF16), pltpu.VMEM(act, BF16), pltpu.VMEM(act, BF16),
                pltpu.VMEM(act[1:], BF16), pltpu.VMEM(act[1:], BF16),
                wide, wide, wide, wide,
                pltpu.VMEM((degrees, hidden, channels), BF16), pltpu.VMEM((hidden, channels), BF16),
                pltpu.VMEM((degrees, hidden, channels), BF16), pltpu.VMEM((tp_size, degrees, share), F32),
                pltpu.VMEM((degrees, channels, hidden), BF16), pltpu.VMEM((channels, hidden), BF16),
                pltpu.VMEM((degrees, channels, hidden), BF16), pltpu.VMEM((degrees, channels, LANES), F32),
                pltpu.VMEM((pts, STEP), BF16), pltpu.VMEM((STEP, pts), BF16), pltpu.VMEM((pts, STEP), BF16), pltpu.VMEM((STEP, pts), BF16),
                pltpu.VMEM((LANES, 2 * LANES), F32), pair, pair, pair, pair,
                pltpu.VMEM((2 * degrees + 1, hidden, channels), F32), pltpu.VMEM((tp_size, 2 * degrees + 1, hid // 2, channels), F32),
                pltpu.VMEM((2, 2 * degrees + 1, hid // 2, channels), F32), pltpu.VMEM((2 * degrees + 1, hid // 2, channels), F32),
                pltpu.VMEM((2 * degrees + 1, hid, channels), BF16),
                pltpu.VMEM(to_grid.shape, F32), pltpu.VMEM(from_grid.shape[::-1], F32),
                dma((3, 4)), dma((3, 4)), dma((2, 4)),
                dma((2,)), dma((2, chunks)), dma((2,)), dma((2,)),
                dma((4,)), dma((4,))],
            compiler_params=pltpu.CompilerParams(collective_id=0, has_side_effects=True, vmem_limit_bytes=48 * 1024 * 1024),
            name='fused',
        )(x_t, g_t, up_t, gate_t, down_loc, gain_loc, to_grid, jnp.transpose(from_grid, (1, 0)))
        out_t, dx_t, d_up, d_gate, d_down = pl.pallas_call(
            write_kernel,
            out_shape=(
                jax.ShapeDtypeStruct(x_t.shape, BF16),
                jax.ShapeDtypeStruct(x_t.shape, BF16),
                jax.ShapeDtypeStruct((degrees, hid, channels), BF16),
                jax.ShapeDtypeStruct((hid, channels), BF16),
                jax.ShapeDtypeStruct((degrees, hid, channels), BF16)),
            in_specs=[vmem] * 3,
            out_specs=(hbm,) * 5,
            scratch_shapes=[dma((5,))],
            compiler_params=pltpu.CompilerParams(vmem_limit_bytes=1024 * 1024),
            name='write',
        )(out_v, dx_v, fin_v)
        back = lambda val: jnp.transpose(val, (2, 0, 1))
        return back(out_t), back(dx_t), jnp.transpose(d_up, (0, 2, 1)), jnp.transpose(d_gate, (1, 0)), d_down

    return jax.shard_map(local_step, mesh=mesh, in_specs=in_specs, out_specs=out_specs, check_vma=False)
```

```python
import jax
import jax.numpy as jnp
from jax import lax
from jax.experimental import pallas as pl
from jax.experimental.pallas import tpu as pltpu
from jax.sharding import PartitionSpec as P

NORM_EPS = 1e-5
F32 = jnp.float32
BF16 = jnp.bfloat16
MESH = pl.DeviceIdType.MESH
LANES = 128
STEP = 56
WIDE = 4


def degree_of(coef):
    total = (coef >= 1).astype(jnp.int32)
    for deg in range(2, 7):
        total = total + (coef >= deg * deg).astype(jnp.int32)
    return total


def mm(lhs, rhs):
    return jnp.dot(lhs, rhs, preferred_element_type=F32)


def mm_nt(lhs, rhs):
    return lax.dot_general(lhs, rhs, (((1,), (1,)), ((), ())), preferred_element_type=F32)


def sigmoid(val):
    return 0.5 * jnp.tanh(0.5 * val) + 0.5


def fused_kernel(x_hbm, g_hbm, up_hbm, gate_hbm, down_hbm, gain_hbm, tg_hbm, fg_hbm,
                 out_vm, dx_vm, fin_vm,
                 x_buf, g_buf, o_buf, n_buf, dn_buf, y0, y1, z0, z1,
                 wu, wg, wd, gain_in, wut, wgt, wdt, gain_b,
                 tt_ref, t_ref, f_ref, ft_ref, pad_buf, u_buf, s_buf, act_buf, du_buf,
                 g_sum, half_buf, mate_buf, far_buf, fin_buf,
                 tg_ref, fg_ref, w_send, w_recv, w_loc, in_send, in_recv, o_send, o_recv, r_send, r_recv, met, row_in):
    chunks, coefs = x_buf.shape[0], x_buf.shape[1]
    share = x_hbm.shape[1]
    own = chunks * LANES
    me = lax.axis_index('tp')
    mate = me ^ 1
    side = lax.axis_index('dp')

    def rows(who, size):
        return pl.ds(pl.multiple_of(who * size, size), size)

    def lanes(who, chunk):
        return pl.ds(pl.multiple_of(who * own + chunk * LANES, LANES), LANES)

    def drain(ref, sem):
        pltpu.make_async_copy(ref, ref, sem).wait()

    barrier = pltpu.get_barrier_semaphore()
    for flip in (1, 2, 3):
        pl.semaphore_signal(barrier, inc=1, device_id={'tp': me ^ flip}, device_id_type=MESH)
    hub = gain_in.shape[0] - 1

    @pl.when(me == hub)
    def _():
        pl.semaphore_signal(barrier, inc=1, device_id={'dp': 1 - side}, device_id_type=MESH)

    pl.semaphore_wait(barrier, 3 + (me == hub).astype(jnp.int32))

    def weight_parts(who):
        hid = up_hbm.shape[1]
        return (wu.at[:, rows(who, hid), :], wd.at[:, rows(who, hid), :], wg.at[rows(who, hid), :], gain_in.at[who])

    sources = (up_hbm, down_hbm, gate_hbm, gain_hbm)

    def weight_copies(srcs, dsts, come, to, peer):
        return [pltpu.make_async_remote_copy(src, dst, w_send.at[to, i], w_recv.at[come, i], device_id=peer, device_id_type=MESH)
                for i, (src, dst) in enumerate(zip(srcs, dsts))]

    crosses = lax.rem(me, 2) == side
    mine, far = weight_parts(me), weight_parts(me ^ 2)
    own_weights = [pltpu.make_async_copy(src, dst, w_loc.at[0, i]) for i, (src, dst) in enumerate(zip(sources, mine))]
    far_weights = weight_copies(sources, mine, 0, 0, {'tp': me ^ 2})
    mate_weights = weight_copies(sources, mine, 1, 1, {'tp': mate})
    passed_weights = (weight_copies(far, far, 2, 2, {'tp': mate}) + weight_copies(far, far, 0, 2, {'dp': 1 - side})
                      + weight_copies(far, far, 2, 2, {'dp': 1 - side, 'tp': mate}))
    hid = up_hbm.shape[1]
    thrice = (wu.at[:, pl.ds(0, 3 * hid), :], wd.at[:, pl.ds(0, 3 * hid), :], wg.at[pl.ds(0, 3 * hid), :], gain_in.at[pl.ds(0, 3)])
    grids = [pltpu.make_async_copy(tg_hbm, tg_ref, w_loc.at[1, 0]), pltpu.make_async_copy(fg_hbm, fg_ref, w_loc.at[1, 1])]

    @pl.when(crosses)
    def _():
        for copy in far_weights:
            copy.start()

    for copy in mate_weights + own_weights + grids:
        copy.start()

    def input_copy(tensor, chunk, flip):
        src, buf = ((x_hbm, x_buf), (g_hbm, g_buf))[tensor]
        return pltpu.make_async_remote_copy(
            src.at[:, :, lanes(me ^ flip, chunk)], buf.at[chunk, :, rows(me, share), :],
            in_send.at[tensor], in_recv.at[tensor, chunk],
            device_id={'tp': me ^ flip}, device_id_type=MESH)

    def input_local(tensor, chunk):
        src, buf = ((x_hbm, x_buf), (g_hbm, g_buf))[tensor]
        return pltpu.make_async_copy(src.at[:, :, lanes(me, chunk)], buf.at[chunk, :, rows(me, share), :], in_recv.at[tensor, chunk])

    def output_copy(tensor, chunk, flip):
        buf, dst = ((o_buf, out_vm), (g_buf, dx_vm))[tensor]
        return pltpu.make_async_remote_copy(
            buf.at[chunk, :, rows(me ^ flip, share), :], dst.at[:, :, lanes(me, chunk)],
            o_send.at[tensor], o_recv.at[tensor],
            device_id={'tp': me ^ flip}, device_id_type=MESH)

    def output_local(tensor, chunk):
        buf, dst = ((o_buf, out_vm), (g_buf, dx_vm))[tensor]
        dst[:, :, lanes(me, chunk)] = buf[chunk, :, rows(me, share), :]

    def start_outputs(tensor, chunk):
        @pl.when(chunk < chunks - 1)
        def _():
            for flip in (2, 3):
                output_copy(tensor, chunk, flip).start()

        output_copy(tensor, chunk, 1).start()
        output_local(tensor, chunk)

    def start_inputs(chunk, carry):
        for flip in (2, 3, 1):
            for tensor in (0, 1):
                input_copy(tensor, chunk, flip).start()
        for tensor in (0, 1):
            input_local(tensor, chunk).start()
        return carry

    lax.fori_loop(0, chunks, start_inputs, 0)

    g_sum[...] = jnp.zeros_like(g_sum)
    blank = jnp.zeros((LANES, LANES), F32)
    for pad in range(coefs, STEP):
        for ref in (y0, y1, z0, z1):
            ref[pl.ds(pad, LANES, stride=STEP), :] = blank
    for ref in (z0, z1):
        ref[pl.ds(0, LANES, stride=STEP), :] = blank

    for copy in grids:
        copy.wait()
    points = tg_ref.shape[1]
    pts = t_ref.shape[1]
    pad_buf[...] = jnp.zeros_like(pad_buf)
    pad_buf[:coefs, :points] = tg_ref[...].astype(BF16).astype(F32)
    t_ref[...] = pad_buf[:STEP, :pts].astype(BF16)
    tt_ref[...] = (0.5 * pad_buf[...]).T[:pts, :STEP].astype(BF16)
    pad_buf[...] = jnp.zeros_like(pad_buf)
    pad_buf[1:coefs, :points] = fg_ref[...].astype(BF16).astype(F32)
    ft_ref[...] = pad_buf[:STEP, :pts].astype(BF16)
    f_ref[...] = (0.5 * pad_buf[...]).T[:pts, :STEP].astype(BF16)

    @pl.when(me == hub)
    def _():
        pl.semaphore_signal(met, inc=1, device_id={'dp': 1 - side}, device_id_type=MESH)
        pl.semaphore_wait(met, 1)
        for flip in (1, 2, 3):
            pl.semaphore_signal(row_in, inc=1, device_id={'tp': me ^ flip}, device_id_type=MESH)

    @pl.when(me != hub)
    def _():
        pl.semaphore_wait(row_in, 1)

    for copy in far_weights:
        copy.wait_recv()

    @pl.when(crosses)
    def _():
        for copy in passed_weights:
            copy.start()
        for i, copy in enumerate(far_weights):
            copy.wait_send()
            drain(thrice[i], w_send.at[2, i])

    for copy in passed_weights[:len(sources)]:
        copy.wait_recv()
    for copy in mate_weights + own_weights:
        copy.wait()

    def turn(deg, carry):
        wut[deg] = wu[deg].astype(F32).T.astype(BF16)
        wdt[deg] = wd[deg].astype(F32).T.astype(BF16)
        return carry

    degrees = wu.shape[0]
    lax.fori_loop(0, degrees, turn, 0)
    wgt[...] = wg[...].astype(F32).T.astype(BF16)
    gains = jnp.concatenate([gain_in[i] for i in range(gain_in.shape[0])], axis=1)
    pad_buf[:degrees, :LANES] = gains
    gains = pad_buf[:, :LANES].T
    for deg in range(degrees):
        gain_b[deg] = jnp.broadcast_to(gains[:, deg:deg + 1], (LANES, LANES))

    inv_chan = 1.0 / LANES
    inv_vec = 1.0 / (LANES * (coefs - 1))

    def chunk_step(chunk, carry):
        for tensor, buf in enumerate((x_buf, g_buf)):
            drain(buf.at[chunk], in_recv.at[tensor, chunk])

        def square_sum(k, acc):
            val = x_buf[chunk, k].astype(F32)
            return acc + val * val

        sq = lax.fori_loop(1, coefs, square_sum, jnp.zeros((LANES, LANES), F32), unroll=8)
        inv_v = lax.rsqrt(jnp.sum(sq, axis=0, keepdims=True) * inv_vec + NORM_EPS)
        scalar = x_buf[chunk, 0].astype(F32)
        cent = scalar - jnp.sum(scalar, axis=0, keepdims=True) * inv_chan
        inv_s = lax.rsqrt(jnp.sum(cent * cent, axis=0, keepdims=True) * inv_chan + NORM_EPS)
        hat_s = cent * inv_s
        n_zero = (hat_s * gain_b[0]).astype(BF16)
        n_buf[0] = n_zero
        y_zero = mm(wu[0], n_zero)
        y0[pl.ds(0, LANES, stride=STEP), :] = y_zero[:LANES]
        y1[pl.ds(0, LANES, stride=STEP), :] = y_zero[LANES:]

        def up_step(k, carry):
            deg = degree_of(k)
            n_k = (x_buf[chunk, k].astype(F32) * inv_v * gain_b[deg]).astype(BF16)
            n_buf[k] = n_k
            y_k = mm(wu[deg], n_k)
            y0[pl.ds(k, LANES, stride=STEP), :] = y_k[:LANES]
            y1[pl.ds(k, LANES, stride=STEP), :] = y_k[LANES:]
            dm_k = mm(wd[deg], g_buf[chunk, k])
            z0[pl.ds(k, LANES, stride=STEP), :] = dm_k[:LANES]
            z1[pl.ds(k, LANES, stride=STEP), :] = dm_k[LANES:]
            return carry

        lax.fori_loop(1, coefs, up_step, 0, unroll=4)

        groups = LANES // WIDE

        def spans_of(group):
            return [pl.ds(pl.multiple_of((group * WIDE + i) * STEP, 8), STEP) for i in range(WIDE)]

        def grid_step(i, carry):
            late = spans_of(jnp.maximum(i - 2, 0))
            early = spans_of(jnp.minimum(i, groups - 1))
            ys = [jnp.concatenate([y0[span, :], y1[span, :]], axis=1).astype(BF16) for span in early]
            dms = [jnp.concatenate([z0[span, :], z1[span, :]], axis=1).astype(BF16) for span in early]
            zs = [mm(ft_ref[...], act_buf[n]) for n in range(WIDE)]
            dys = [mm(t_ref[...], du_buf[n]) for n in range(WIDE)]
            for n in range(WIDE):
                half = u_buf[n].astype(F32)
                tan = jnp.tanh(half)
                both = half * tan
                act_buf[n] = (half + both).astype(BF16)
                du_buf[n] = (s_buf[n].astype(F32) * ((1.0 + tan) + (half - both * tan))).astype(BF16)
            for n in range(WIDE):
                u_buf[n] = mm(tt_ref[...], ys[n]).astype(BF16)
                s_buf[n] = mm(f_ref[...], dms[n]).astype(BF16)
            for span, z_j, dy_j in zip(late, zs, dys):
                z0[span, :] = z_j[:, :LANES]
                z1[span, :] = z_j[:, LANES:]
                y0[span, :] = dy_j[:, :LANES]
                y1[span, :] = dy_j[:, LANES:]
            return carry

        lax.fori_loop(0, groups + 2, grid_step, 0)

        def hidden_grad(k):
            picked = pl.ds(k, LANES, stride=STEP)
            return jnp.concatenate([y0[picked, :], y1[picked, :]], axis=0).astype(BF16)

        g_zero = g_buf[chunk, 0]
        n_zero = n_buf[0]
        pre = mm(wg[...], n_zero).astype(BF16).astype(F32)
        sig = sigmoid(pre)
        gate = pre * sig
        dm_zero = mm(wd[0], g_zero).astype(BF16).astype(F32)
        d_pre = (dm_zero * (sig + gate * (1.0 - sig))).astype(BF16)
        gate = gate.astype(BF16)
        o_buf[chunk, 0] = (x_buf[chunk, 0].astype(F32) + mm(wdt[0], gate)).astype(BF16)
        g_sum[degrees] += mm_nt(gate, g_zero)
        dy_zero = hidden_grad(0)
        g_sum[0] += mm_nt(dy_zero, n_zero)
        g_sum[2 * degrees] += mm_nt(d_pre, n_zero)
        dn_zero = (mm(wut[0], dy_zero) + mm(wgt[...], d_pre)).astype(BF16).astype(F32)

        def down_step(k, acc):
            deg = degree_of(k)
            picked = pl.ds(k, LANES, stride=STEP)
            m_k = jnp.concatenate([z0[picked, :], z1[picked, :]], axis=0).astype(BF16)
            dy_k = hidden_grad(k)
            x_k = x_buf[chunk, k].astype(F32)
            o_buf[chunk, k] = (x_k + mm(wdt[deg], m_k)).astype(BF16)
            g_sum[degrees + deg] += mm_nt(m_k, g_buf[chunk, k])
            dn_k = mm(wut[deg], dy_k).astype(BF16)
            dn_buf[k] = dn_k
            g_sum[deg] += mm_nt(dy_k, n_buf[k])
            return acc + dn_k.astype(F32) * gain_b[deg] * x_k

        dot_v = lax.fori_loop(1, coefs, down_step, jnp.zeros((LANES, LANES), F32), unroll=4)
        start_outputs(0, chunk)

        z0[pl.ds(0, LANES, stride=STEP), :] = blank
        z1[pl.ds(0, LANES, stride=STEP), :] = blank
        dh_s = dn_zero * gain_b[0]
        mean_d = jnp.sum(dh_s, axis=0, keepdims=True) * inv_chan
        mean_dx = jnp.sum(dh_s * hat_s, axis=0, keepdims=True) * inv_chan
        dx_s = inv_s * (dh_s - mean_d - hat_s * mean_dx)
        g_buf[chunk, 0] = (dx_s + g_zero.astype(F32)).astype(BF16)
        coef_v = inv_v * inv_v * inv_v * (jnp.sum(dot_v, axis=0, keepdims=True) * inv_vec)

        def back_step(k, carry):
            dh = dn_buf[k].astype(F32) * gain_b[degree_of(k)]
            dx = inv_v * dh - x_buf[chunk, k].astype(F32) * coef_v
            g_buf[chunk, k] = (dx + g_buf[chunk, k].astype(F32)).astype(BF16)
            return carry

        lax.fori_loop(1, coefs, back_step, 0, unroll=4)
        start_outputs(1, chunk)
        return carry

    lax.fori_loop(0, chunks, chunk_step, 0)

    part = hid // 2
    slices = half_buf.shape[0]

    def sum_rows(who, where):
        return pl.ds(pl.multiple_of(who * hid + where * part, part), part)

    def push(src, dst, num, peer):
        return pltpu.make_async_remote_copy(src, dst, r_send.at[num], r_recv.at[num], device_id=peer, device_id_type=MESH)

    for n in range(slices):
        push(g_sum.at[:, sum_rows(n, 1 - side), :], half_buf.at[n], 0, {'dp': 1 - side}).start()
    drain(half_buf, r_recv.at[0])
    rows_all = g_sum.shape[0]

    def add_half(row, carry):
        for n in range(slices):
            half_buf[n, row] += g_sum[row, sum_rows(n, side), :]
        return carry

    lax.fori_loop(0, rows_all, add_half, 0)
    push(half_buf.at[mate], mate_buf.at[0], 1, {'tp': mate}).start()
    push(half_buf.at[mate ^ 2], mate_buf.at[1], 1, {'tp': mate}).start()
    drain(mate_buf, r_recv.at[1])
    drain(mate_buf, r_send.at[1])

    def add_mate(row, carry):
        mate_buf[0, row] += half_buf[me, row]
        mate_buf[1, row] += half_buf[me ^ 2, row]
        return carry

    lax.fori_loop(0, rows_all, add_mate, 0)
    cross = push(mate_buf.at[1], far_buf, 2, {'tp': me ^ 2})
    cross.start()
    for tensor in (0, 1):
        for flip in (2, 3):
            output_copy(tensor, chunks - 1, flip).start()
    cross.wait()
    ours = pl.ds(pl.multiple_of(side * part, part), part)

    def add_far(row, carry):
        fin_buf[row, ours, :] = (mate_buf[0, row] + far_buf[row]).astype(BF16)
        return carry

    lax.fori_loop(0, rows_all, add_far, 0)
    last = push(fin_buf.at[:, ours, :], fin_buf.at[:, ours, :], 3, {'dp': 1 - side})
    last.start()
    last.wait()
    drain(half_buf, r_send.at[0])
    fin_vm[...] = fin_buf[...]

    for tensor, (buf, dst) in enumerate(((o_buf, out_vm), (g_buf, dx_vm))):
        sent = buf.at[:, :, pl.ds(0, LANES - share), :]
        drain(sent, in_send.at[tensor])
        drain(sent, o_send.at[tensor])
        drain(dst.at[:, :, pl.ds(0, x_hbm.shape[2] - own)], o_recv.at[tensor])


def write_kernel(out_vm, dx_vm, fin_vm, out_hbm, dx_hbm, dup_hbm, dgate_hbm, ddown_hbm, sems):
    coefs, step = out_hbm.shape[0], 7
    degrees = dup_hbm.shape[0]
    for start in range(0, coefs, step):
        span = pl.ds(start, step)
        pltpu.make_async_copy(out_vm.at[span], out_hbm.at[span], sems.at[0]).start()
        pltpu.make_async_copy(dx_vm.at[span], dx_hbm.at[span], sems.at[1]).start()
    small = [pltpu.make_async_copy(fin_vm.at[pl.ds(0, degrees)], dup_hbm, sems.at[2]),
             pltpu.make_async_copy(fin_vm.at[pl.ds(degrees, degrees)], ddown_hbm, sems.at[3]),
             pltpu.make_async_copy(fin_vm.at[2 * degrees], dgate_hbm, sems.at[4])]
    for copy in small:
        copy.start()
    for copy in small:
        copy.wait()
    pltpu.make_async_copy(out_vm, out_hbm, sems.at[0]).wait()
    pltpu.make_async_copy(dx_vm, dx_hbm, sems.at[1]).wait()


def solution(mesh):
    tp_size = mesh.shape['tp']
    act_spec = P('dp', None, 'tp')
    in_specs = (act_spec, P(None, 'tp'), P(None, None, 'tp'), P(None, 'tp'), P(None, 'tp', None), P(None, None), P(None, None), act_spec)
    out_specs = (act_spec, act_spec, P(None, None, 'tp'), P(None, 'tp'), P(None, 'tp', None))

    def local_step(x_loc, gain_loc, up_loc, gate_loc, down_loc, to_grid, from_grid, grad_loc):
        nodes, coefs, share = x_loc.shape
        degrees, channels, hid = up_loc.shape
        hidden = hid * tp_size
        points = to_grid.shape[1]
        pts = -(-points // 8) * 8
        chunks = nodes // tp_size // LANES
        x_t = jnp.transpose(x_loc, (1, 2, 0))
        g_t = jnp.transpose(grad_loc, (1, 2, 0))
        up_t = jnp.transpose(up_loc, (0, 2, 1))
        gate_t = jnp.transpose(gate_loc, (1, 0))
        hbm = pl.BlockSpec(memory_space=pl.ANY)
        vmem = pl.BlockSpec(memory_space=pltpu.VMEM)
        dma = pltpu.SemaphoreType.DMA
        act = (chunks, coefs, channels, LANES)
        wide = pltpu.VMEM((LANES * STEP, LANES), F32)
        pair = pltpu.VMEM((WIDE, pts, 2 * LANES), BF16)
        out_v, dx_v, fin_v = pl.pallas_call(
            fused_kernel,
            out_shape=(pltpu.VMEM(x_t.shape, BF16), pltpu.VMEM(x_t.shape, BF16), pltpu.VMEM((2 * degrees + 1, hid, channels), BF16)),
            in_specs=[hbm] * 8,
            out_specs=(vmem, vmem, vmem),
            scratch_shapes=[
                pltpu.VMEM(act, BF16), pltpu.VMEM(act, BF16), pltpu.VMEM(act, BF16),
                pltpu.VMEM(act[1:], BF16), pltpu.VMEM(act[1:], BF16),
                wide, wide, wide, wide,
                pltpu.VMEM((degrees, hidden, channels), BF16), pltpu.VMEM((hidden, channels), BF16),
                pltpu.VMEM((degrees, hidden, channels), BF16), pltpu.VMEM((tp_size, degrees, share), F32),
                pltpu.VMEM((degrees, channels, hidden), BF16), pltpu.VMEM((channels, hidden), BF16),
                pltpu.VMEM((degrees, channels, hidden), BF16), pltpu.VMEM((degrees, channels, LANES), F32),
                pltpu.VMEM((pts, STEP), BF16), pltpu.VMEM((STEP, pts), BF16), pltpu.VMEM((pts, STEP), BF16), pltpu.VMEM((STEP, pts), BF16),
                pltpu.VMEM((LANES, 2 * LANES), F32), pair, pair, pair, pair,
                pltpu.VMEM((2 * degrees + 1, hidden, channels), F32), pltpu.VMEM((tp_size, 2 * degrees + 1, hid // 2, channels), F32),
                pltpu.VMEM((2, 2 * degrees + 1, hid // 2, channels), F32), pltpu.VMEM((2 * degrees + 1, hid // 2, channels), F32),
                pltpu.VMEM((2 * degrees + 1, hid, channels), BF16),
                pltpu.VMEM(to_grid.shape, F32), pltpu.VMEM(from_grid.shape[::-1], F32),
                dma((3, 4)), dma((3, 4)), dma((2, 4)),
                dma((2,)), dma((2, chunks)), dma((2,)), dma((2,)),
                dma((4,)), dma((4,)), pltpu.SemaphoreType.REGULAR, pltpu.SemaphoreType.REGULAR],
            compiler_params=pltpu.CompilerParams(collective_id=0, has_side_effects=True, vmem_limit_bytes=48 * 1024 * 1024),
            name='fused',
        )(x_t, g_t, up_t, gate_t, down_loc, gain_loc, to_grid, jnp.transpose(from_grid, (1, 0)))
        out_t, dx_t, d_up, d_gate, d_down = pl.pallas_call(
            write_kernel,
            out_shape=(
                jax.ShapeDtypeStruct(x_t.shape, BF16),
                jax.ShapeDtypeStruct(x_t.shape, BF16),
                jax.ShapeDtypeStruct((degrees, hid, channels), BF16),
                jax.ShapeDtypeStruct((hid, channels), BF16),
                jax.ShapeDtypeStruct((degrees, hid, channels), BF16)),
            in_specs=[vmem] * 3,
            out_specs=(hbm,) * 5,
            scratch_shapes=[dma((5,))],
            compiler_params=pltpu.CompilerParams(vmem_limit_bytes=1024 * 1024),
            name='write',
        )(out_v, dx_v, fin_v)
        back = lambda val: jnp.transpose(val, (2, 0, 1))
        return back(out_t), back(dx_t), jnp.transpose(d_up, (0, 2, 1)), jnp.transpose(d_gate, (1, 0)), d_down

    return jax.shard_map(local_step, mesh=mesh, in_specs=in_specs, out_specs=out_specs, check_vma=False)
```

```python
import jax
import jax.numpy as jnp
from jax import lax
from jax.experimental import pallas as pl
from jax.experimental.pallas import tpu as pltpu
from jax.sharding import PartitionSpec as P

NORM_EPS = 1e-5
F32 = jnp.float32
BF16 = jnp.bfloat16
MESH = pl.DeviceIdType.MESH
LANES = 128
STEP = 56
WIDE = 4


def degree_of(coef):
    total = (coef >= 1).astype(jnp.int32)
    for deg in range(2, 7):
        total = total + (coef >= deg * deg).astype(jnp.int32)
    return total


def mm(lhs, rhs):
    return jnp.dot(lhs, rhs, preferred_element_type=F32)


def mm_nt(lhs, rhs):
    return lax.dot_general(lhs, rhs, (((1,), (1,)), ((), ())), preferred_element_type=F32)


def sigmoid(val):
    return 0.5 * jnp.tanh(0.5 * val) + 0.5


def fused_kernel(x_hbm, g_hbm, up_hbm, gate_hbm, down_hbm, gain_hbm, tg_hbm, fg_hbm,
                 out_vm, dx_vm, fin_vm,
                 x_buf, g_buf, o_buf, n_buf, dn_buf, y0, y1, z0, z1,
                 wu, wg, wd, gain_in, wut, wgt, wdt, gain_b,
                 tt_ref, t_ref, f_ref, ft_ref, pad_buf, u_buf, s_buf, act_buf, du_buf,
                 g_sum, half_buf, mate_buf, far_buf, fin_buf,
                 tg_ref, fg_ref, w_send, w_recv, w_loc, in_send, in_recv, o_send, o_recv, r_send, r_recv, met, row_in):
    chunks, coefs = x_buf.shape[0], x_buf.shape[1]
    share = x_hbm.shape[1]
    own = chunks * LANES
    me = lax.axis_index('tp')
    mate = me ^ 1
    side = lax.axis_index('dp')

    def rows(who, size):
        return pl.ds(pl.multiple_of(who * size, size), size)

    def lanes(who, chunk):
        return pl.ds(pl.multiple_of(who * own + chunk * LANES, LANES), LANES)

    def drain(ref, sem):
        pltpu.make_async_copy(ref, ref, sem).wait()

    barrier = pltpu.get_barrier_semaphore()
    for flip in (1, 2, 3):
        pl.semaphore_signal(barrier, inc=1, device_id={'tp': me ^ flip}, device_id_type=MESH)
    hub = gain_in.shape[0] - 2

    @pl.when(me == hub)
    def _():
        pl.semaphore_signal(barrier, inc=1, device_id={'dp': 1 - side}, device_id_type=MESH)

    pl.semaphore_wait(barrier, 3 + (me == hub).astype(jnp.int32))

    def weight_parts(who):
        hid = up_hbm.shape[1]
        return (wu.at[:, rows(who, hid), :], wd.at[:, rows(who, hid), :], wg.at[rows(who, hid), :], gain_in.at[who])

    sources = (up_hbm, down_hbm, gate_hbm, gain_hbm)

    def weight_copies(srcs, dsts, come, to, peer):
        return [pltpu.make_async_remote_copy(src, dst, w_send.at[to, i // 3], w_recv.at[come, i // 3], device_id=peer, device_id_type=MESH)
                for i, (src, dst) in enumerate(zip(srcs, dsts))]

    crosses = lax.rem(me, 2) == side
    mine, far = weight_parts(me), weight_parts(me ^ 2)
    own_weights = [pltpu.make_async_copy(src, dst, w_recv.at[1, i // 3]) for i, (src, dst) in enumerate(zip(sources, mine))]
    far_weights = weight_copies(sources, mine, 0, 1, {'tp': me ^ 2})
    mate_weights = weight_copies(sources, mine, 1, 0, {'tp': mate})
    passed_weights = (weight_copies(far, far, 1, 1, {'tp': mate}) + weight_copies(far, far, 0, 1, {'dp': 1 - side})
                      + weight_copies(far, far, 1, 1, {'dp': 1 - side, 'tp': mate}))
    hid = up_hbm.shape[1]
    grids = [pltpu.make_async_copy(tg_hbm, tg_ref, w_loc.at[0]), pltpu.make_async_copy(fg_hbm, fg_ref, w_loc.at[1])]

    def drain_slices(count, sem):
        drain(n_buf.at[pl.ds(0, count * fin_buf.shape[0] // 2 if count % 2 == 0 else count * fin_buf.shape[0]),
                       pl.ds(0, LANES if count % 2 == 0 else hid), :], sem.at[0])
        drain(gain_in.at[pl.ds(0, count)], sem.at[1])

    @pl.when(crosses)
    def _():
        for copy in far_weights:
            copy.start()

    for copy in mate_weights + own_weights + grids:
        copy.start()

    def input_copy(tensor, chunk, flip):
        src, buf = ((x_hbm, x_buf), (g_hbm, g_buf))[tensor]
        return pltpu.make_async_remote_copy(
            src.at[:, :, lanes(me ^ flip, chunk)], buf.at[chunk, :, rows(me, share), :],
            in_send.at[tensor], in_recv.at[chunk],
            device_id={'tp': me ^ flip}, device_id_type=MESH)

    def input_local(tensor, chunk):
        src, buf = ((x_hbm, x_buf), (g_hbm, g_buf))[tensor]
        return pltpu.make_async_copy(src.at[:, :, lanes(me, chunk)], buf.at[chunk, :, rows(me, share), :], in_recv.at[chunk])

    def output_copy(tensor, chunk, flip):
        buf, dst = ((o_buf, out_vm), (g_buf, dx_vm))[tensor]
        return pltpu.make_async_remote_copy(
            buf.at[chunk, :, rows(me ^ flip, share), :], dst.at[:, :, lanes(me, chunk)],
            o_send.at[tensor], o_recv.at[tensor],
            device_id={'tp': me ^ flip}, device_id_type=MESH)

    def output_local(tensor, chunk):
        buf, dst = ((o_buf, out_vm), (g_buf, dx_vm))[tensor]
        dst[:, :, lanes(me, chunk)] = buf[chunk, :, rows(me, share), :]

    def start_outputs(tensor, chunk):
        @pl.when(chunk < chunks - 1)
        def _():
            for flip in (2, 3):
                output_copy(tensor, chunk, flip).start()

        output_copy(tensor, chunk, 1).start()
        output_local(tensor, chunk)

    def start_inputs(chunk, carry):
        for flip in (2, 3, 1):
            for tensor in (0, 1):
                input_copy(tensor, chunk, flip).start()
        for tensor in (0, 1):
            input_local(tensor, chunk).start()
        return carry

    lax.fori_loop(0, chunks, start_inputs, 0)

    g_sum[...] = jnp.zeros_like(g_sum)
    blank = jnp.zeros((LANES, LANES), F32)
    for pad in range(coefs, STEP):
        for ref in (y0, y1, z0, z1):
            ref[pl.ds(pad, LANES, stride=STEP), :] = blank
    for ref in (z0, z1):
        ref[pl.ds(0, LANES, stride=STEP), :] = blank

    for copy in grids:
        copy.wait()
    points = tg_ref.shape[1]
    pts = t_ref.shape[1]
    pad_buf[...] = jnp.zeros_like(pad_buf)
    pad_buf[:coefs, :points] = tg_ref[...].astype(BF16).astype(F32)
    t_ref[...] = pad_buf[:STEP, :pts].astype(BF16)
    tt_ref[...] = (0.5 * pad_buf[...]).T[:pts, :STEP].astype(BF16)
    pad_buf[...] = jnp.zeros_like(pad_buf)
    pad_buf[1:coefs, :points] = fg_ref[...].astype(BF16).astype(F32)
    ft_ref[...] = pad_buf[:STEP, :pts].astype(BF16)
    f_ref[...] = (0.5 * pad_buf[...]).T[:pts, :STEP].astype(BF16)

    @pl.when(me == hub)
    def _():
        pl.semaphore_signal(met, inc=1, device_id={'dp': 1 - side}, device_id_type=MESH)
        pl.semaphore_wait(met, 1)
        for flip in (1, 2, 3):
            pl.semaphore_signal(row_in, inc=1, device_id={'tp': me ^ flip}, device_id_type=MESH)

    @pl.when(me != hub)
    def _():
        pl.semaphore_wait(row_in, 1)

    drain_slices(1, w_recv.at[0])

    @pl.when(crosses)
    def _():
        for copy in passed_weights:
            copy.start()
        drain_slices(4, w_send.at[1])

    drain_slices(3, w_recv.at[1])
    drain_slices(1, w_send.at[0])

    def turn(deg, carry):
        wut[deg] = wu[deg].astype(F32).T.astype(BF16)
        wdt[deg] = wd[deg].astype(F32).T.astype(BF16)
        return carry

    degrees = wu.shape[0]
    lax.fori_loop(0, degrees, turn, 0)
    wgt[...] = wg[...].astype(F32).T.astype(BF16)
    gains = jnp.concatenate([gain_in[i] for i in range(gain_in.shape[0])], axis=1)
    pad_buf[:degrees, :LANES] = gains
    gains = pad_buf[:, :LANES].T
    for deg in range(degrees):
        gain_b[deg] = jnp.broadcast_to(gains[:, deg:deg + 1], (LANES, LANES))

    inv_chan = 1.0 / LANES
    inv_vec = 1.0 / (LANES * (coefs - 1))

    def chunk_step(chunk, carry):
        drain(x_buf.at[pl.ds(0, 2)], in_recv.at[chunk])

        def square_sum(k, acc):
            val = x_buf[chunk, k].astype(F32)
            return acc + val * val

        sq = lax.fori_loop(1, coefs, square_sum, jnp.zeros((LANES, LANES), F32), unroll=8)
        inv_v = lax.rsqrt(jnp.sum(sq, axis=0, keepdims=True) * inv_vec + NORM_EPS)
        scalar = x_buf[chunk, 0].astype(F32)
        cent = scalar - jnp.sum(scalar, axis=0, keepdims=True) * inv_chan
        inv_s = lax.rsqrt(jnp.sum(cent * cent, axis=0, keepdims=True) * inv_chan + NORM_EPS)
        hat_s = cent * inv_s
        n_zero = (hat_s * gain_b[0]).astype(BF16)
        n_buf[0] = n_zero
        y_zero = mm(wu[0], n_zero)
        y0[pl.ds(0, LANES, stride=STEP), :] = y_zero[:LANES]
        y1[pl.ds(0, LANES, stride=STEP), :] = y_zero[LANES:]

        def up_step(k, carry):
            deg = degree_of(k)
            n_k = (x_buf[chunk, k].astype(F32) * inv_v * gain_b[deg]).astype(BF16)
            n_buf[k] = n_k
            y_k = mm(wu[deg], n_k)
            y0[pl.ds(k, LANES, stride=STEP), :] = y_k[:LANES]
            y1[pl.ds(k, LANES, stride=STEP), :] = y_k[LANES:]
            dm_k = mm(wd[deg], g_buf[chunk, k])
            z0[pl.ds(k, LANES, stride=STEP), :] = dm_k[:LANES]
            z1[pl.ds(k, LANES, stride=STEP), :] = dm_k[LANES:]
            return carry

        lax.fori_loop(1, coefs, up_step, 0, unroll=4)

        groups = LANES // WIDE

        def spans_of(group):
            return [pl.ds(pl.multiple_of((group * WIDE + i) * STEP, 8), STEP) for i in range(WIDE)]

        def grid_step(i, carry):
            late = spans_of(jnp.maximum(i - 2, 0))
            early = spans_of(jnp.minimum(i, groups - 1))
            ys = [jnp.concatenate([y0[span, :], y1[span, :]], axis=1).astype(BF16) for span in early]
            dms = [jnp.concatenate([z0[span, :], z1[span, :]], axis=1).astype(BF16) for span in early]
            zs = [mm(ft_ref[...], act_buf[n]) for n in range(WIDE)]
            dys = [mm(t_ref[...], du_buf[n]) for n in range(WIDE)]
            for n in range(WIDE):
                half = u_buf[n].astype(F32)
                tan = jnp.tanh(half)
                both = half * tan
                act_buf[n] = (half + both).astype(BF16)
                du_buf[n] = (s_buf[n].astype(F32) * ((1.0 + tan) + (half - both * tan))).astype(BF16)
            for n in range(WIDE):
                u_buf[n] = mm(tt_ref[...], ys[n]).astype(BF16)
                s_buf[n] = mm(f_ref[...], dms[n]).astype(BF16)
            for span, z_j, dy_j in zip(late, zs, dys):
                z0[span, :] = z_j[:, :LANES]
                z1[span, :] = z_j[:, LANES:]
                y0[span, :] = dy_j[:, :LANES]
                y1[span, :] = dy_j[:, LANES:]
            return carry

        lax.fori_loop(0, groups + 2, grid_step, 0)

        def hidden_grad(k):
            picked = pl.ds(k, LANES, stride=STEP)
            return jnp.concatenate([y0[picked, :], y1[picked, :]], axis=0).astype(BF16)

        g_zero = g_buf[chunk, 0]
        n_zero = n_buf[0]
        pre = mm(wg[...], n_zero).astype(BF16).astype(F32)
        sig = sigmoid(pre)
        gate = pre * sig
        dm_zero = mm(wd[0], g_zero).astype(BF16).astype(F32)
        d_pre = (dm_zero * (sig + gate * (1.0 - sig))).astype(BF16)
        gate = gate.astype(BF16)
        o_buf[chunk, 0] = (x_buf[chunk, 0].astype(F32) + mm(wdt[0], gate)).astype(BF16)
        g_sum[degrees] += mm_nt(gate, g_zero)
        dy_zero = hidden_grad(0)
        g_sum[0] += mm_nt(dy_zero, n_zero)
        g_sum[2 * degrees] += mm_nt(d_pre, n_zero)
        dn_zero = (mm(wut[0], dy_zero) + mm(wgt[...], d_pre)).astype(BF16).astype(F32)

        def down_step(k, acc):
            deg = degree_of(k)
            picked = pl.ds(k, LANES, stride=STEP)
            m_k = jnp.concatenate([z0[picked, :], z1[picked, :]], axis=0).astype(BF16)
            dy_k = hidden_grad(k)
            x_k = x_buf[chunk, k].astype(F32)
            o_buf[chunk, k] = (x_k + mm(wdt[deg], m_k)).astype(BF16)
            g_sum[degrees + deg] += mm_nt(m_k, g_buf[chunk, k])
            dn_k = mm(wut[deg], dy_k).astype(BF16)
            dn_buf[k] = dn_k
            g_sum[deg] += mm_nt(dy_k, n_buf[k])
            return acc + dn_k.astype(F32) * gain_b[deg] * x_k

        dot_v = lax.fori_loop(1, coefs, down_step, jnp.zeros((LANES, LANES), F32), unroll=4)
        start_outputs(0, chunk)

        z0[pl.ds(0, LANES, stride=STEP), :] = blank
        z1[pl.ds(0, LANES, stride=STEP), :] = blank
        dh_s = dn_zero * gain_b[0]
        mean_d = jnp.sum(dh_s, axis=0, keepdims=True) * inv_chan
        mean_dx = jnp.sum(dh_s * hat_s, axis=0, keepdims=True) * inv_chan
        dx_s = inv_s * (dh_s - mean_d - hat_s * mean_dx)
        g_buf[chunk, 0] = (dx_s + g_zero.astype(F32)).astype(BF16)
        coef_v = inv_v * inv_v * inv_v * (jnp.sum(dot_v, axis=0, keepdims=True) * inv_vec)

        def back_step(k, carry):
            dh = dn_buf[k].astype(F32) * gain_b[degree_of(k)]
            dx = inv_v * dh - x_buf[chunk, k].astype(F32) * coef_v
            g_buf[chunk, k] = (dx + g_buf[chunk, k].astype(F32)).astype(BF16)
            return carry

        lax.fori_loop(1, coefs, back_step, 0, unroll=4)
        start_outputs(1, chunk)
        return carry

    lax.fori_loop(0, chunks, chunk_step, 0)

    part = hid // 2
    slices = half_buf.shape[0]

    def sum_rows(who, where):
        return pl.ds(pl.multiple_of(who * hid + where * part, part), part)

    def push(src, dst, num, peer):
        return pltpu.make_async_remote_copy(src, dst, r_send, r_recv.at[num], device_id=peer, device_id_type=MESH)

    for n in range(slices):
        push(g_sum.at[:, sum_rows(n, 1 - side), :], half_buf.at[n], 0, {'dp': 1 - side}).start()
    drain(half_buf, r_recv.at[0])
    rows_all = g_sum.shape[0]

    def add_half(row, carry):
        for n in range(slices):
            half_buf[n, row] += g_sum[row, sum_rows(n, side), :]
        return carry

    lax.fori_loop(0, rows_all, add_half, 0)
    push(half_buf.at[mate], mate_buf.at[0], 1, {'tp': mate}).start()
    push(half_buf.at[mate ^ 2], mate_buf.at[1], 1, {'tp': mate}).start()
    drain(mate_buf, r_recv.at[1])

    def add_mate(row, carry):
        mate_buf[0, row] += half_buf[me, row]
        mate_buf[1, row] += half_buf[me ^ 2, row]
        return carry

    lax.fori_loop(0, rows_all, add_mate, 0)
    cross = push(mate_buf.at[1], far_buf, 2, {'tp': me ^ 2})
    cross.start()
    for tensor in (0, 1):
        for flip in (2, 3):
            output_copy(tensor, chunks - 1, flip).start()
    cross.wait_recv()
    ours = pl.ds(pl.multiple_of(side * part, part), part)

    def add_far(row, carry):
        fin_buf[row, ours, :] = (mate_buf[0, row] + far_buf[row]).astype(BF16)
        return carry

    lax.fori_loop(0, rows_all, add_far, 0)
    last = push(fin_buf.at[:, ours, :], fin_buf.at[:, ours, :], 3, {'dp': 1 - side})
    last.start()
    last.wait_recv()
    drain(g_sum.at[:, pl.ds(0, slices * hid * 15 // 16), :], r_send)
    fin_vm[...] = fin_buf[...]

    for tensor, (buf, dst) in enumerate(((o_buf, out_vm), (g_buf, dx_vm))):
        sent = buf.at[:, :, pl.ds(0, LANES - share), :]
        drain(sent, in_send.at[tensor])
        drain(sent, o_send.at[tensor])
        drain(dst.at[:, :, pl.ds(0, x_hbm.shape[2] - own)], o_recv.at[tensor])


def write_kernel(out_vm, dx_vm, fin_vm, out_hbm, dx_hbm, dup_hbm, dgate_hbm, ddown_hbm, sems):
    coefs, step = out_hbm.shape[0], 1
    degrees = dup_hbm.shape[0]
    for start in range(0, coefs, step):
        span = pl.ds(start, step)
        pltpu.make_async_copy(out_vm.at[span], out_hbm.at[span], sems.at[0]).start()
        pltpu.make_async_copy(dx_vm.at[span], dx_hbm.at[span], sems.at[1]).start()
    pltpu.make_async_copy(fin_vm.at[pl.ds(0, degrees)], dup_hbm, sems.at[2]).start()
    pltpu.make_async_copy(fin_vm.at[pl.ds(degrees, degrees)], ddown_hbm, sems.at[2]).start()
    pltpu.make_async_copy(fin_vm.at[2 * degrees], dgate_hbm, sems.at[2]).start()
    pltpu.make_async_copy(fin_vm, fin_vm, sems.at[2]).wait()
    pltpu.make_async_copy(out_vm, out_hbm, sems.at[0]).wait()
    pltpu.make_async_copy(dx_vm, dx_hbm, sems.at[1]).wait()


def solution(mesh):
    tp_size = mesh.shape['tp']
    act_spec = P('dp', None, 'tp')
    in_specs = (act_spec, P(None, 'tp'), P(None, None, 'tp'), P(None, 'tp'), P(None, 'tp', None), P(None, None), P(None, None), act_spec)
    out_specs = (act_spec, act_spec, P(None, None, 'tp'), P(None, 'tp'), P(None, 'tp', None))

    def local_step(x_loc, gain_loc, up_loc, gate_loc, down_loc, to_grid, from_grid, grad_loc):
        nodes, coefs, share = x_loc.shape
        degrees, channels, hid = up_loc.shape
        hidden = hid * tp_size
        points = to_grid.shape[1]
        pts = -(-points // 8) * 8
        chunks = nodes // tp_size // LANES
        x_t = jnp.transpose(x_loc, (1, 2, 0))
        g_t = jnp.transpose(grad_loc, (1, 2, 0))
        up_t = jnp.transpose(up_loc, (0, 2, 1))
        gate_t = jnp.transpose(gate_loc, (1, 0))
        hbm = pl.BlockSpec(memory_space=pl.ANY)
        vmem = pl.BlockSpec(memory_space=pltpu.VMEM)
        dma = pltpu.SemaphoreType.DMA
        act = (chunks, coefs, channels, LANES)
        wide = pltpu.VMEM((LANES * STEP, LANES), F32)
        pair = pltpu.VMEM((WIDE, pts, 2 * LANES), BF16)
        out_v, dx_v, fin_v = pl.pallas_call(
            fused_kernel,
            out_shape=(pltpu.VMEM(x_t.shape, BF16), pltpu.VMEM(x_t.shape, BF16), pltpu.VMEM((2 * degrees + 1, hid, channels), BF16)),
            in_specs=[hbm] * 8,
            out_specs=(vmem, vmem, vmem),
            scratch_shapes=[
                pltpu.VMEM(act, BF16), pltpu.VMEM(act, BF16), pltpu.VMEM(act, BF16),
                pltpu.VMEM(act[1:], BF16), pltpu.VMEM(act[1:], BF16),
                wide, wide, wide, wide,
                pltpu.VMEM((degrees, hidden, channels), BF16), pltpu.VMEM((hidden, channels), BF16),
                pltpu.VMEM((degrees, hidden, channels), BF16), pltpu.VMEM((tp_size, degrees, share), F32),
                pltpu.VMEM((degrees, channels, hidden), BF16), pltpu.VMEM((channels, hidden), BF16),
                pltpu.VMEM((degrees, channels, hidden), BF16), pltpu.VMEM((degrees, channels, LANES), F32),
                pltpu.VMEM((pts, STEP), BF16), pltpu.VMEM((STEP, pts), BF16), pltpu.VMEM((pts, STEP), BF16), pltpu.VMEM((STEP, pts), BF16),
                pltpu.VMEM((LANES, 2 * LANES), F32), pair, pair, pair, pair,
                pltpu.VMEM((2 * degrees + 1, hidden, channels), F32), pltpu.VMEM((tp_size, 2 * degrees + 1, hid // 2, channels), F32),
                pltpu.VMEM((2, 2 * degrees + 1, hid // 2, channels), F32), pltpu.VMEM((2 * degrees + 1, hid // 2, channels), F32),
                pltpu.VMEM((2 * degrees + 1, hid, channels), BF16),
                pltpu.VMEM(to_grid.shape, F32), pltpu.VMEM(from_grid.shape[::-1], F32),
                dma((2, 2)), dma((2, 2)), dma((2,)),
                dma((2,)), dma((chunks,)), dma((2,)), dma((2,)),
                dma(()), dma((4,)), pltpu.SemaphoreType.REGULAR, pltpu.SemaphoreType.REGULAR],
            compiler_params=pltpu.CompilerParams(collective_id=0, has_side_effects=True, vmem_limit_bytes=48 * 1024 * 1024),
            name='fused',
        )(x_t, g_t, up_t, gate_t, down_loc, gain_loc, to_grid, jnp.transpose(from_grid, (1, 0)))
        out_t, dx_t, d_up, d_gate, d_down = pl.pallas_call(
            write_kernel,
            out_shape=(
                jax.ShapeDtypeStruct(x_t.shape, BF16),
                jax.ShapeDtypeStruct(x_t.shape, BF16),
                jax.ShapeDtypeStruct((degrees, hid, channels), BF16),
                jax.ShapeDtypeStruct((hid, channels), BF16),
                jax.ShapeDtypeStruct((degrees, hid, channels), BF16)),
            in_specs=[vmem] * 3,
            out_specs=(hbm,) * 5,
            scratch_shapes=[dma((3,))],
            compiler_params=pltpu.CompilerParams(vmem_limit_bytes=1024 * 1024),
            name='write',
        )(out_v, dx_v, fin_v)
        back = lambda val: jnp.transpose(val, (2, 0, 1))
        return back(out_t), back(dx_t), jnp.transpose(d_up, (0, 2, 1)), jnp.transpose(d_gate, (1, 0)), d_down

    return jax.shard_map(local_step, mesh=mesh, in_specs=in_specs, out_specs=out_specs, check_vma=False)
```

```python
import jax
import jax.numpy as jnp
from jax import lax
from jax.experimental import pallas as pl
from jax.experimental.pallas import tpu as pltpu
from jax.sharding import PartitionSpec as P

NORM_EPS = 1e-5
F32 = jnp.float32
BF16 = jnp.bfloat16
MESH = pl.DeviceIdType.MESH
LANES = 128
STEP = 56
WIDE = 4


def degree_of(coef):
    total = (coef >= 1).astype(jnp.int32)
    for deg in range(2, 7):
        total = total + (coef >= deg * deg).astype(jnp.int32)
    return total


def mm(lhs, rhs):
    return jnp.dot(lhs, rhs, preferred_element_type=F32)


def mm_nt(lhs, rhs):
    return lax.dot_general(lhs, rhs, (((1,), (1,)), ((), ())), preferred_element_type=F32)


def sigmoid(val):
    return 0.5 * jnp.tanh(0.5 * val) + 0.5


def fused_kernel(x_hbm, g_hbm, up_hbm, gate_hbm, down_hbm, gain_hbm, tg_hbm, fg_hbm,
                 out_vm, dx_vm, fin_vm,
                 x_buf, g_buf, o_buf, n_buf, dn_buf, y0, y1, z0, z1,
                 wu, wg, wd, gain_in, wut, wgt, wdt, gain_b,
                 tt_ref, t_ref, f_ref, ft_ref, pad_buf, u_buf, s_buf, act_buf, du_buf,
                 g_sum, half_buf, mate_buf, far_buf, fin_buf,
                 tg_ref, fg_ref, w_send, w_recv, w_loc, in_send, in_recv, o_send, o_recv, r_send, r_recv, met, row_in):
    chunks, coefs = x_buf.shape[0], x_buf.shape[1]
    share = x_hbm.shape[1]
    own = chunks * LANES
    me = lax.axis_index('tp')
    mate = me ^ 1
    side = lax.axis_index('dp')

    def rows(who, size):
        return pl.ds(pl.multiple_of(who * size, size), size)

    def lanes(who, chunk):
        return pl.ds(pl.multiple_of(who * own + chunk * LANES, LANES), LANES)

    def drain(ref, sem):
        pltpu.make_async_copy(ref, ref, sem).wait()

    barrier = pltpu.get_barrier_semaphore()
    for flip in (1, 2, 3):
        pl.semaphore_signal(barrier, inc=1, device_id={'tp': me ^ flip}, device_id_type=MESH)
    hub = gain_in.shape[0] - 2

    @pl.when(me == hub)
    def _():
        pl.semaphore_signal(barrier, inc=1, device_id={'dp': 1 - side}, device_id_type=MESH)

    pl.semaphore_wait(barrier, 3 + (me == hub).astype(jnp.int32))

    def weight_parts(who):
        hid = up_hbm.shape[1]
        return (wu.at[:, rows(who, hid), :], wd.at[:, rows(who, hid), :], wg.at[rows(who, hid), :], gain_in.at[who])

    sources = (up_hbm, down_hbm, gate_hbm, gain_hbm)

    def weight_copies(srcs, dsts, come, to, peer):
        return [pltpu.make_async_remote_copy(src, dst, w_send.at[to, i // 3], w_recv.at[come, i // 3], device_id=peer, device_id_type=MESH)
                for i, (src, dst) in enumerate(zip(srcs, dsts))]

    crosses = lax.rem(me, 2) != side
    mine, far = weight_parts(me), weight_parts(me ^ 2)
    own_weights = [pltpu.make_async_copy(src, dst, w_recv.at[1, i // 3]) for i, (src, dst) in enumerate(zip(sources, mine))]
    far_weights = weight_copies(sources, mine, 0, 1, {'tp': me ^ 2})
    mate_weights = weight_copies(sources, mine, 1, 0, {'tp': mate})
    passed_weights = (weight_copies(far, far, 1, 1, {'tp': mate}) + weight_copies(far, far, 0, 1, {'dp': 1 - side})
                      + weight_copies(far, far, 1, 1, {'dp': 1 - side, 'tp': mate}))
    hid = up_hbm.shape[1]
    grids = [pltpu.make_async_copy(tg_hbm, tg_ref, w_loc.at[0]), pltpu.make_async_copy(fg_hbm, fg_ref, w_loc.at[1])]

    def drain_slices(count, sem):
        drain(n_buf.at[pl.ds(0, count * fin_buf.shape[0] // 2 if count % 2 == 0 else count * fin_buf.shape[0]),
                       pl.ds(0, LANES if count % 2 == 0 else hid), :], sem.at[0])
        drain(gain_in.at[pl.ds(0, count)], sem.at[1])

    @pl.when(crosses)
    def _():
        for copy in far_weights:
            copy.start()

    for copy in mate_weights + own_weights + grids:
        copy.start()

    def input_copy(tensor, chunk, flip):
        src, buf = ((x_hbm, x_buf), (g_hbm, g_buf))[tensor]
        return pltpu.make_async_remote_copy(
            src.at[:, :, lanes(me ^ flip, chunk)], buf.at[chunk, :, rows(me, share), :],
            in_send.at[tensor], in_recv.at[chunk],
            device_id={'tp': me ^ flip}, device_id_type=MESH)

    def input_local(tensor, chunk):
        src, buf = ((x_hbm, x_buf), (g_hbm, g_buf))[tensor]
        return pltpu.make_async_copy(src.at[:, :, lanes(me, chunk)], buf.at[chunk, :, rows(me, share), :], in_recv.at[chunk])

    def output_copy(tensor, chunk, flip):
        buf, dst = ((o_buf, out_vm), (g_buf, dx_vm))[tensor]
        return pltpu.make_async_remote_copy(
            buf.at[chunk, :, rows(me ^ flip, share), :], dst.at[:, :, lanes(me, chunk)],
            o_send.at[tensor], o_recv.at[tensor],
            device_id={'tp': me ^ flip}, device_id_type=MESH)

    def output_local(tensor, chunk):
        buf, dst = ((o_buf, out_vm), (g_buf, dx_vm))[tensor]
        dst[:, :, lanes(me, chunk)] = buf[chunk, :, rows(me, share), :]

    def start_outputs(tensor, chunk):
        @pl.when(chunk < chunks - 1)
        def _():
            for flip in (2, 3):
                output_copy(tensor, chunk, flip).start()

        output_copy(tensor, chunk, 1).start()
        output_local(tensor, chunk)

    def start_inputs(chunk, carry):
        for flip in (2, 3, 1):
            for tensor in (0, 1):
                input_copy(tensor, chunk, flip).start()
        for tensor in (0, 1):
            input_local(tensor, chunk).start()
        return carry

    lax.fori_loop(0, chunks, start_inputs, 0)

    g_sum[...] = jnp.zeros_like(g_sum)
    blank = jnp.zeros((LANES, LANES), F32)
    for pad in range(coefs, STEP):
        for ref in (y0, y1, z0, z1):
            ref[pl.ds(pad, LANES, stride=STEP), :] = blank
    for ref in (z0, z1):
        ref[pl.ds(0, LANES, stride=STEP), :] = blank

    for copy in grids:
        copy.wait()
    points = tg_ref.shape[1]
    pts = t_ref.shape[1]
    pad_buf[...] = jnp.zeros_like(pad_buf)
    pad_buf[:coefs, :points] = tg_ref[...].astype(BF16).astype(F32)
    t_ref[...] = pad_buf[:STEP, :pts].astype(BF16)
    tt_ref[...] = (0.5 * pad_buf[...]).T[:pts, :STEP].astype(BF16)
    pad_buf[...] = jnp.zeros_like(pad_buf)
    pad_buf[1:coefs, :points] = fg_ref[...].astype(BF16).astype(F32)
    ft_ref[...] = pad_buf[:STEP, :pts].astype(BF16)
    f_ref[...] = (0.5 * pad_buf[...]).T[:pts, :STEP].astype(BF16)

    @pl.when(me == hub)
    def _():
        pl.semaphore_signal(met, inc=1, device_id={'dp': 1 - side}, device_id_type=MESH)
        pl.semaphore_wait(met, 1)
        for flip in (1, 2, 3):
            pl.semaphore_signal(row_in, inc=1, device_id={'tp': me ^ flip}, device_id_type=MESH)

    @pl.when(me != hub)
    def _():
        pl.semaphore_wait(row_in, 1)

    drain_slices(1, w_recv.at[0])

    @pl.when(crosses)
    def _():
        for copy in passed_weights:
            copy.start()
        drain_slices(4, w_send.at[1])

    drain_slices(3, w_recv.at[1])
    drain_slices(1, w_send.at[0])

    def turn(deg, carry):
        wut[deg] = wu[deg].astype(F32).T.astype(BF16)
        wdt[deg] = wd[deg].astype(F32).T.astype(BF16)
        return carry

    degrees = wu.shape[0]
    lax.fori_loop(0, degrees, turn, 0)
    wgt[...] = wg[...].astype(F32).T.astype(BF16)
    gains = jnp.concatenate([gain_in[i] for i in range(gain_in.shape[0])], axis=1)
    pad_buf[:degrees, :LANES] = gains
    gains = pad_buf[:, :LANES].T
    for deg in range(degrees):
        gain_b[deg] = jnp.broadcast_to(gains[:, deg:deg + 1], (LANES, LANES))

    inv_chan = 1.0 / LANES
    inv_vec = 1.0 / (LANES * (coefs - 1))

    def chunk_step(chunk, carry):
        drain(x_buf.at[pl.ds(0, 2)], in_recv.at[chunk])

        def square_sum(k, acc):
            val = x_buf[chunk, k].astype(F32)
            return acc + val * val

        sq = lax.fori_loop(1, coefs, square_sum, jnp.zeros((LANES, LANES), F32), unroll=8)
        inv_v = lax.rsqrt(jnp.sum(sq, axis=0, keepdims=True) * inv_vec + NORM_EPS)
        scalar = x_buf[chunk, 0].astype(F32)
        cent = scalar - jnp.sum(scalar, axis=0, keepdims=True) * inv_chan
        inv_s = lax.rsqrt(jnp.sum(cent * cent, axis=0, keepdims=True) * inv_chan + NORM_EPS)
        hat_s = cent * inv_s
        n_zero = (hat_s * gain_b[0]).astype(BF16)
        n_buf[0] = n_zero
        y_zero = mm(wu[0], n_zero)
        y0[pl.ds(0, LANES, stride=STEP), :] = y_zero[:LANES]
        y1[pl.ds(0, LANES, stride=STEP), :] = y_zero[LANES:]

        def up_step(k, carry):
            deg = degree_of(k)
            n_k = (x_buf[chunk, k].astype(F32) * inv_v * gain_b[deg]).astype(BF16)
            n_buf[k] = n_k
            y_k = mm(wu[deg], n_k)
            y0[pl.ds(k, LANES, stride=STEP), :] = y_k[:LANES]
            y1[pl.ds(k, LANES, stride=STEP), :] = y_k[LANES:]
            dm_k = mm(wd[deg], g_buf[chunk, k])
            z0[pl.ds(k, LANES, stride=STEP), :] = dm_k[:LANES]
            z1[pl.ds(k, LANES, stride=STEP), :] = dm_k[LANES:]
            return carry

        lax.fori_loop(1, coefs, up_step, 0, unroll=4)

        groups = LANES // WIDE

        def spans_of(group):
            return [pl.ds(pl.multiple_of((group * WIDE + i) * STEP, 8), STEP) for i in range(WIDE)]

        def grid_step(i, carry):
            late = spans_of(jnp.maximum(i - 2, 0))
            early = spans_of(jnp.minimum(i, groups - 1))
            ys = [jnp.concatenate([y0[span, :], y1[span, :]], axis=1).astype(BF16) for span in early]
            dms = [jnp.concatenate([z0[span, :], z1[span, :]], axis=1).astype(BF16) for span in early]
            zs = [mm(ft_ref[...], act_buf[n]) for n in range(WIDE)]
            dys = [mm(t_ref[...], du_buf[n]) for n in range(WIDE)]
            for n in range(WIDE):
                half = u_buf[n].astype(F32)
                tan = jnp.tanh(half)
                both = half * tan
                act_buf[n] = (half + both).astype(BF16)
                du_buf[n] = (s_buf[n].astype(F32) * ((1.0 + tan) + (half - both * tan))).astype(BF16)
            for n in range(WIDE):
                u_buf[n] = mm(tt_ref[...], ys[n]).astype(BF16)
                s_buf[n] = mm(f_ref[...], dms[n]).astype(BF16)
            for span, z_j, dy_j in zip(late, zs, dys):
                z0[span, :] = z_j[:, :LANES]
                z1[span, :] = z_j[:, LANES:]
                y0[span, :] = dy_j[:, :LANES]
                y1[span, :] = dy_j[:, LANES:]
            return carry

        lax.fori_loop(0, groups + 2, grid_step, 0)

        def hidden_grad(k):
            picked = pl.ds(k, LANES, stride=STEP)
            return jnp.concatenate([y0[picked, :], y1[picked, :]], axis=0).astype(BF16)

        g_zero = g_buf[chunk, 0]
        n_zero = n_buf[0]
        pre = mm(wg[...], n_zero).astype(BF16).astype(F32)
        sig = sigmoid(pre)
        gate = pre * sig
        dm_zero = mm(wd[0], g_zero).astype(BF16).astype(F32)
        d_pre = (dm_zero * (sig + gate * (1.0 - sig))).astype(BF16)
        gate = gate.astype(BF16)
        o_buf[chunk, 0] = (x_buf[chunk, 0].astype(F32) + mm(wdt[0], gate)).astype(BF16)
        g_sum[degrees] += mm_nt(gate, g_zero)
        dy_zero = hidden_grad(0)
        g_sum[0] += mm_nt(dy_zero, n_zero)
        g_sum[2 * degrees] += mm_nt(d_pre, n_zero)
        dn_zero = (mm(wut[0], dy_zero) + mm(wgt[...], d_pre)).astype(BF16).astype(F32)

        def down_step(k, acc):
            deg = degree_of(k)
            picked = pl.ds(k, LANES, stride=STEP)
            m_k = jnp.concatenate([z0[picked, :], z1[picked, :]], axis=0).astype(BF16)
            dy_k = hidden_grad(k)
            x_k = x_buf[chunk, k].astype(F32)
            o_buf[chunk, k] = (x_k + mm(wdt[deg], m_k)).astype(BF16)
            g_sum[degrees + deg] += mm_nt(m_k, g_buf[chunk, k])
            dn_k = mm(wut[deg], dy_k).astype(BF16)
            dn_buf[k] = dn_k
            g_sum[deg] += mm_nt(dy_k, n_buf[k])
            return acc + dn_k.astype(F32) * gain_b[deg] * x_k

        dot_v = lax.fori_loop(1, coefs, down_step, jnp.zeros((LANES, LANES), F32), unroll=4)
        start_outputs(0, chunk)

        z0[pl.ds(0, LANES, stride=STEP), :] = blank
        z1[pl.ds(0, LANES, stride=STEP), :] = blank
        dh_s = dn_zero * gain_b[0]
        mean_d = jnp.sum(dh_s, axis=0, keepdims=True) * inv_chan
        mean_dx = jnp.sum(dh_s * hat_s, axis=0, keepdims=True) * inv_chan
        dx_s = inv_s * (dh_s - mean_d - hat_s * mean_dx)
        g_buf[chunk, 0] = (dx_s + g_zero.astype(F32)).astype(BF16)
        coef_v = inv_v * inv_v * inv_v * (jnp.sum(dot_v, axis=0, keepdims=True) * inv_vec)

        def back_step(k, carry):
            dh = dn_buf[k].astype(F32) * gain_b[degree_of(k)]
            dx = inv_v * dh - x_buf[chunk, k].astype(F32) * coef_v
            g_buf[chunk, k] = (dx + g_buf[chunk, k].astype(F32)).astype(BF16)
            return carry

        lax.fori_loop(1, coefs, back_step, 0, unroll=4)
        start_outputs(1, chunk)
        return carry

    lax.fori_loop(0, chunks, chunk_step, 0)

    part = hid // 2
    slices = half_buf.shape[0]

    def sum_rows(who, where):
        return pl.ds(pl.multiple_of(who * hid + where * part, part), part)

    def push(src, dst, num, peer):
        return pltpu.make_async_remote_copy(src, dst, r_send, r_recv.at[num], device_id=peer, device_id_type=MESH)

    for n in range(slices):
        push(g_sum.at[:, sum_rows(n, 1 - side), :], half_buf.at[n], 0, {'dp': 1 - side}).start()
    drain(half_buf, r_recv.at[0])
    rows_all = g_sum.shape[0]

    def add_half(row, carry):
        for n in range(slices):
            half_buf[n, row] += g_sum[row, sum_rows(n, side), :]
        return carry

    lax.fori_loop(0, rows_all, add_half, 0)
    push(half_buf.at[mate], mate_buf.at[0], 1, {'tp': mate}).start()
    push(half_buf.at[mate ^ 2], mate_buf.at[1], 1, {'tp': mate}).start()
    drain(mate_buf, r_recv.at[1])

    def add_mate(row, carry):
        mate_buf[0, row] += half_buf[me, row]
        mate_buf[1, row] += half_buf[me ^ 2, row]
        return carry

    lax.fori_loop(0, rows_all, add_mate, 0)
    cross = push(mate_buf.at[1], far_buf, 2, {'tp': me ^ 2})
    cross.start()
    for tensor in (0, 1):
        for flip in (3, 2):
            output_copy(tensor, chunks - 1, flip).start()
    cross.wait_recv()
    ours = pl.ds(pl.multiple_of(side * part, part), part)

    def add_far(row, carry):
        fin_buf[row, ours, :] = (mate_buf[0, row] + far_buf[row]).astype(BF16)
        return carry

    lax.fori_loop(0, rows_all, add_far, 0)
    last = push(fin_buf.at[:, ours, :], fin_buf.at[:, ours, :], 3, {'dp': 1 - side})
    last.start()
    last.wait_recv()
    drain(g_sum.at[:, pl.ds(0, slices * hid * 15 // 16), :], r_send)
    fin_vm[...] = fin_buf[...]

    for tensor, (buf, dst) in enumerate(((o_buf, out_vm), (g_buf, dx_vm))):
        sent = buf.at[:, :, pl.ds(0, LANES - share), :]
        drain(sent, in_send.at[tensor])
        drain(sent, o_send.at[tensor])
        drain(dst.at[:, :, pl.ds(0, x_hbm.shape[2] - own)], o_recv.at[tensor])


def write_kernel(out_vm, dx_vm, fin_vm, out_hbm, dx_hbm, dup_hbm, dgate_hbm, ddown_hbm, sems):
    coefs, step = out_hbm.shape[0], 1
    degrees = dup_hbm.shape[0]
    for start in range(0, coefs, step):
        span = pl.ds(start, step)
        pltpu.make_async_copy(out_vm.at[span], out_hbm.at[span], sems.at[0]).start()
        pltpu.make_async_copy(dx_vm.at[span], dx_hbm.at[span], sems.at[1]).start()
    pltpu.make_async_copy(fin_vm.at[pl.ds(0, degrees)], dup_hbm, sems.at[2]).start()
    pltpu.make_async_copy(fin_vm.at[pl.ds(degrees, degrees)], ddown_hbm, sems.at[2]).start()
    pltpu.make_async_copy(fin_vm.at[2 * degrees], dgate_hbm, sems.at[2]).start()
    pltpu.make_async_copy(fin_vm, fin_vm, sems.at[2]).wait()
    pltpu.make_async_copy(out_vm, out_hbm, sems.at[0]).wait()
    pltpu.make_async_copy(dx_vm, dx_hbm, sems.at[1]).wait()


def solution(mesh):
    tp_size = mesh.shape['tp']
    act_spec = P('dp', None, 'tp')
    in_specs = (act_spec, P(None, 'tp'), P(None, None, 'tp'), P(None, 'tp'), P(None, 'tp', None), P(None, None), P(None, None), act_spec)
    out_specs = (act_spec, act_spec, P(None, None, 'tp'), P(None, 'tp'), P(None, 'tp', None))

    def local_step(x_loc, gain_loc, up_loc, gate_loc, down_loc, to_grid, from_grid, grad_loc):
        nodes, coefs, share = x_loc.shape
        degrees, channels, hid = up_loc.shape
        hidden = hid * tp_size
        points = to_grid.shape[1]
        pts = -(-points // 8) * 8
        chunks = nodes // tp_size // LANES
        x_t = jnp.transpose(x_loc, (1, 2, 0))
        g_t = jnp.transpose(grad_loc, (1, 2, 0))
        up_t = jnp.transpose(up_loc, (0, 2, 1))
        gate_t = jnp.transpose(gate_loc, (1, 0))
        hbm = pl.BlockSpec(memory_space=pl.ANY)
        vmem = pl.BlockSpec(memory_space=pltpu.VMEM)
        dma = pltpu.SemaphoreType.DMA
        act = (chunks, coefs, channels, LANES)
        wide = pltpu.VMEM((LANES * STEP, LANES), F32)
        pair = pltpu.VMEM((WIDE, pts, 2 * LANES), BF16)
        out_v, dx_v, fin_v = pl.pallas_call(
            fused_kernel,
            out_shape=(pltpu.VMEM(x_t.shape, BF16), pltpu.VMEM(x_t.shape, BF16), pltpu.VMEM((2 * degrees + 1, hid, channels), BF16)),
            in_specs=[hbm] * 8,
            out_specs=(vmem, vmem, vmem),
            scratch_shapes=[
                pltpu.VMEM(act, BF16), pltpu.VMEM(act, BF16), pltpu.VMEM(act, BF16),
                pltpu.VMEM(act[1:], BF16), pltpu.VMEM(act[1:], BF16),
                wide, wide, wide, wide,
                pltpu.VMEM((degrees, hidden, channels), BF16), pltpu.VMEM((hidden, channels), BF16),
                pltpu.VMEM((degrees, hidden, channels), BF16), pltpu.VMEM((tp_size, degrees, share), F32),
                pltpu.VMEM((degrees, channels, hidden), BF16), pltpu.VMEM((channels, hidden), BF16),
                pltpu.VMEM((degrees, channels, hidden), BF16), pltpu.VMEM((degrees, channels, LANES), F32),
                pltpu.VMEM((pts, STEP), BF16), pltpu.VMEM((STEP, pts), BF16), pltpu.VMEM((pts, STEP), BF16), pltpu.VMEM((STEP, pts), BF16),
                pltpu.VMEM((LANES, 2 * LANES), F32), pair, pair, pair, pair,
                pltpu.VMEM((2 * degrees + 1, hidden, channels), F32), pltpu.VMEM((tp_size, 2 * degrees + 1, hid // 2, channels), F32),
                pltpu.VMEM((2, 2 * degrees + 1, hid // 2, channels), F32), pltpu.VMEM((2 * degrees + 1, hid // 2, channels), F32),
                pltpu.VMEM((2 * degrees + 1, hid, channels), BF16),
                pltpu.VMEM(to_grid.shape, F32), pltpu.VMEM(from_grid.shape[::-1], F32),
                dma((2, 2)), dma((2, 2)), dma((2,)),
                dma((2,)), dma((chunks,)), dma((2,)), dma((2,)),
                dma(()), dma((4,)), pltpu.SemaphoreType.REGULAR, pltpu.SemaphoreType.REGULAR],
            compiler_params=pltpu.CompilerParams(collective_id=0, has_side_effects=True, vmem_limit_bytes=48 * 1024 * 1024),
            name='fused',
        )(x_t, g_t, up_t, gate_t, down_loc, gain_loc, to_grid, jnp.transpose(from_grid, (1, 0)))
        out_t, dx_t, d_up, d_gate, d_down = pl.pallas_call(
            write_kernel,
            out_shape=(
                jax.ShapeDtypeStruct(x_t.shape, BF16),
                jax.ShapeDtypeStruct(x_t.shape, BF16),
                jax.ShapeDtypeStruct((degrees, hid, channels), BF16),
                jax.ShapeDtypeStruct((hid, channels), BF16),
                jax.ShapeDtypeStruct((degrees, hid, channels), BF16)),
            in_specs=[vmem] * 3,
            out_specs=(hbm,) * 5,
            scratch_shapes=[dma((3,))],
            compiler_params=pltpu.CompilerParams(vmem_limit_bytes=1024 * 1024),
            name='write',
        )(out_v, dx_v, fin_v)
        back = lambda val: jnp.transpose(val, (2, 0, 1))
        return back(out_t), back(dx_t), jnp.transpose(d_up, (0, 2, 1)), jnp.transpose(d_gate, (1, 0)), d_down

    return jax.shard_map(local_step, mesh=mesh, in_specs=in_specs, out_specs=out_specs, check_vma=False)
```
